8 devices in a mesh: dp: 2 (over z, y), tp: 4 (over x, core).
Axes of the slice: x: 2, y: 2, z: 1, core: 2. Of those that a mesh axis runs over, the one named last changes fastest.
Arguments:
- x: bfloat16 [2, 2048, 512], P('dp', 'tp')
- dy: bfloat16 [2, 2048, 512], P('dp', 'tp')
- wq: bfloat16 [512, 8192], P('dp', 'tp')
- wk: bfloat16 [512, 8192], P('dp', 'tp')
- wv: bfloat16 [512, 8192], P('dp', 'tp')
- wo: bfloat16 [8192, 512], P(('tp', 'dp'))
- w_gate: bfloat16 [512, 32768], P('dp', 'tp')
- w_up: bfloat16 [512, 32768], P('dp', 'tp')
- w_down: bfloat16 [32768, 512], P(('tp', 'dp'))
Outputs:
- output 1: bfloat16 [2, 2048, 512], P('dp', 'tp')
- output 2: bfloat16 [512, 8192], P('dp', 'tp')
- output 3: bfloat16 [512, 8192], P('dp', 'tp')
- output 4: bfloat16 [512, 8192], P('dp', 'tp')
- output 5: bfloat16 [8192, 512], P(('tp', 'dp'))
- output 6: bfloat16 [512, 32768], P('dp', 'tp')
- output 7: bfloat16 [512, 32768], P('dp', 'tp')
- output 8: bfloat16 [32768, 512], P(('tp', 'dp'))
All inputs are finite; a program needn't handle non-finite values.
Results may differ from the reference program's by a relative error of at most 0.024.
Values are sent between devices in bfloat16 or wider.
A program may use at most 2 GiB of HBM per device.

```python
import jax
import jax.numpy as jnp
from jax import lax

SEQUENCES = 2
TOKENS = 2048
D = 512
HEADS = 64
KV_HEADS = 64
HEAD = 128
FF = 32768
THETA = 10000
NAMES = ("wq", "wk", "wv", "wo", "w_gate", "w_up", "w_down")
SHAPES = {
    "wq": (D, HEADS * HEAD),
    "wk": (D, KV_HEADS * HEAD),
    "wv": (D, KV_HEADS * HEAD),
    "wo": (HEADS * HEAD, D),
    "w_gate": (D, FF),
    "w_up": (D, FF),
    "w_down": (FF, D),
}


def bump(key, n, height):
    away = (jnp.arange(n, dtype=jnp.int32) - jax.random.randint(key, (), 0, n, jnp.int32)) % n
    return jnp.where(away < n // 8, height, 1.0)


def together(key, own, strength):
    shared = jax.random.normal(key, own.shape[1:], jnp.float32)
    return (own + strength * shared) * lax.rsqrt(1 + strength * strength)


def setup_inputs(seed: int = 0, part: int = 0) -> dict:
    kx, kdy, ka, kb, kz, kf, kh, kl, *kw = jax.random.split(jax.random.key(seed), 8 + len(NAMES))
    shape = (SEQUENCES, TOKENS, D)
    much_x, much_dy = jax.random.uniform(kz, (2,), jnp.float32, 0.0, 1.0)
    loud = 2.0 ** jax.random.uniform(jax.random.fold_in(kz, 1), (), jnp.float32, -1.0, 2.0)
    halves = 2.0 ** jax.random.uniform(kl, (2,), jnp.float32, -1.0, 1.0)
    times = {"wq": 1.0, "wk": 1.0, "wv": 2.0, "wo": halves[0], "w_gate": 1.0, "w_up": bump(kh, FF, 4.0), "w_down": halves[1]}
    x = together(ka, jax.random.normal(kx, shape, jnp.float32), much_x) * bump(kf, D, 4.0)
    dy = together(kb, jax.random.normal(kdy, shape, jnp.float32), much_dy)
    drawn = {"x": x.astype(jnp.bfloat16), "dy": (loud * dy * (SEQUENCES * TOKENS) ** -0.5).astype(jnp.bfloat16)}
    for key, name in zip(kw, NAMES, strict=True):
        drawn[name] = (jax.random.normal(key, SHAPES[name], jnp.float32) * SHAPES[name][0] ** -0.5 * times[name]).astype(jnp.bfloat16)
    return drawn


def matmul(a, w):
    return jnp.dot(a, w, preferred_element_type=jnp.float32).astype(jnp.bfloat16)


def normed(h):
    wide = h.astype(jnp.float32)
    scale = lax.rsqrt(jnp.mean(wide**2, -1, keepdims=True) + 1e-6)
    return (wide * scale).astype(jnp.bfloat16)


def turned(t, theta):
    half = t.shape[-1] // 2
    angle = jnp.arange(t.shape[0], dtype=jnp.float32)[:, None] * theta ** (-jnp.arange(half, dtype=jnp.float32) / half)
    cos, sin = jnp.cos(angle)[:, None], jnp.sin(angle)[:, None]
    a, b = t[..., :half].astype(jnp.float32), t[..., half:].astype(jnp.float32)
    return jnp.concatenate([a * cos - b * sin, b * cos + a * sin], -1).astype(jnp.bfloat16)


def seen_by(q, k, v):
    tokens, kv = q.shape[0], k.shape[1]
    q = q.reshape(tokens, kv, -1, q.shape[-1])
    scores = jnp.einsum("tgsd,ugd->gstu", q.astype(jnp.float32), k.astype(jnp.float32)) * q.shape[-1] ** -0.5
    place = jnp.arange(tokens)
    weights = jax.nn.softmax(jnp.where(place[:, None] >= place, scores, -jnp.inf), -1).astype(jnp.bfloat16)
    return jnp.einsum("gstu,ugd->tgsd", weights.astype(jnp.float32), v.astype(jnp.float32)).astype(jnp.bfloat16).reshape(tokens, -1)


def layer(h, w):
    a = normed(h)
    q, k = (turned(matmul(a, w[name]).reshape(h.shape[0], -1, HEAD), THETA) for name in ("wq", "wk"))
    h = h + matmul(seen_by(q, k, matmul(a, w["wv"]).reshape(h.shape[0], -1, HEAD)), w["wo"])
    b = normed(h)
    gate = jnp.dot(b, w["w_gate"], preferred_element_type=jnp.float32)
    up = jnp.dot(b, w["w_up"], preferred_element_type=jnp.float32)
    return h + matmul((jax.nn.silu(gate) * up).astype(jnp.bfloat16), w["w_down"])


def reference(x, dy, wq, wk, wv, wo, w_gate, w_up, w_down):
    weights = dict(zip(NAMES, (wq, wk, wv, wo, w_gate, w_up, w_down), strict=True))

    def take(so_far, sequence):
        h, by_y = sequence
        _, back = jax.vjp(lambda w, h: layer(h, w), weights, h)
        by_weights, by_h = back(by_y)
        return jax.tree.map(lambda total, term: total + term.astype(jnp.float32), so_far, by_weights), by_h

    none_yet = {name: jnp.zeros(w.shape, jnp.float32) for name, w in weights.items()}
    by_weights, by_x = lax.scan(take, none_yet, (x, dy))
    return (by_x, *(by_weights[name].astype(jnp.bfloat16) for name in NAMES))
```

```python
import functools

import jax
import jax.numpy as jnp
from jax import lax
from jax.experimental import pallas as pl
from jax.experimental.pallas import tpu as pltpu
from jax.sharding import PartitionSpec as P

HEAD = 128
THETA = 10000
NAMES = ("wq", "wk", "wv", "wo", "w_gate", "w_up", "w_down")
NEG = -1e30
HIDDEN = 2 * NEG
LOG2E = 1.4426950408889634
VMEM = 60 * 2**20
BF, F32 = jnp.bfloat16, jnp.float32


def _dot(a, b, ca=1, cb=0):
    return lax.dot_general(a, b, (((ca,), (cb,)), ((), ())), preferred_element_type=F32)


def _params(*kinds):
    return pltpu.CompilerParams(dimension_semantics=kinds, vmem_limit_bytes=VMEM)


def _head(i):
    return slice(i * HEAD, (i + 1) * HEAD)


def _qkv(a_ref, qo, qr, ko, kr, vo, vr, cos_ref, sin_ref, q_ref, k_ref, v_ref, *, rows):
    depth = qo.shape[0]

    def some(n, _):
        here = pl.ds(pl.multiple_of(n * rows, rows), rows)
        a = a_ref[here, :]
        cos, sin = cos_ref[here, :], sin_ref[here, :]
        for own, other, out, turn in ((qo, qr, q_ref, True), (ko, kr, k_ref, True), (vo, vr, v_ref, False)):
            t = (_dot(a[:, :depth], own[...]) + _dot(a[:, depth:], other[...])).astype(BF)
            for h in range(out.shape[1] // HEAD):
                u = t[:, _head(h)]
                if turn:
                    u = u.astype(F32)
                    u = (u * cos + pltpu.roll(u, HEAD // 2, 1) * sin).astype(BF)
                out[here, _head(h)] = u

    lax.fori_loop(0, a_ref.shape[0] // rows, some, None)


def qkv(a, ws, cos, sin, wide=256, rows=512):
    tokens, d = a.shape
    cols = ws[0].shape[1]
    whole = lambda *shape: pl.BlockSpec(shape, lambda n: (0, 0))
    w = pl.BlockSpec((d // 2, wide), lambda n: (0, n))
    out = pl.BlockSpec((tokens, wide), lambda n: (0, n))
    return pl.pallas_call(
        functools.partial(_qkv, rows=rows),
        grid=(cols // wide,),
        in_specs=[whole(tokens, d), *[w] * 6, whole(tokens, HEAD), whole(tokens, HEAD)],
        out_specs=[out] * 3,
        out_shape=[jax.ShapeDtypeStruct((tokens, cols), BF)] * 3,
        compiler_params=_params("arbitrary"),
        cost_estimate=pl.CostEstimate(flops=6 * tokens * d * cols, transcendentals=0, bytes_accessed=2 * (tokens * d + 3 * d * cols + 3 * tokens * cols)),
        name="qkv",
    )(a, *ws, cos, sin)


def _below(bk, bq):
    return lax.broadcasted_iota(jnp.int32, (bk, bq), 1) >= lax.broadcasted_iota(jnp.int32, (bk, bq), 0)


def _attend(q_ref, k_ref, v_ref, o_ref, lse_ref, top_s, mix_s, *, kb, bq, scale):
    iq = pl.program_id(1)
    e = scale * LOG2E
    top_s[...] = jnp.full(top_s.shape, NEG, F32)
    mix_s[...] = jnp.zeros(mix_s.shape, F32)
    ones = jnp.ones((8, bq), BF)

    def block(j, masked):
        here = pl.ds(pl.multiple_of(j * bq, bq), bq)
        scores = [_dot(k_ref[here, _head(i)], q_ref[:, _head(i)], 1, 1) for i in range(kb)]
        ok = _below(bq, bq) if masked else None
        weights, keeps = [], []
        for i, s in enumerate(scores):
            if masked:
                s = jnp.where(ok, s, HIDDEN)
            old = top_s[i : i + 1, :]
            top = jnp.maximum(old, s.max(axis=0, keepdims=True))
            top_s[i : i + 1, :] = top
            weights.append(jnp.exp2((s - top) * e).astype(BF))
            keeps.append(jnp.exp2((old - top) * e))
        for i in range(kb):
            values = jnp.concatenate([v_ref[here, _head(i)].T, ones], axis=0)
            mix_s[i] = mix_s[i] * keeps[i] + _dot(values, weights[i])

    lax.fori_loop(0, iq, lambda j, _: block(j, False), None)
    block(iq, True)
    for i in range(kb):
        top, total = top_s[i : i + 1, :], mix_s[i, HEAD : HEAD + 1, :]
        o_ref[:, _head(i)] = (mix_s[i, :HEAD, :] * (1 / total)).T.astype(BF)
        lse_ref[i : i + 1, :] = top * scale + jnp.log(total)


def attend(q, k, v, kb=8, bq=512):
    tokens, cols = q.shape
    heads = cols // HEAD
    some = pl.BlockSpec((bq, kb * HEAD), lambda h, n: (n, h))
    keys = pl.BlockSpec((tokens, kb * HEAD), lambda h, n: (0, h))
    return pl.pallas_call(
        functools.partial(_attend, kb=kb, bq=bq, scale=HEAD**-0.5),
        grid=(heads // kb, tokens // bq),
        in_specs=[some, keys, keys],
        out_specs=[some, pl.BlockSpec((kb, bq), lambda h, n: (h, n))],
        out_shape=[jax.ShapeDtypeStruct(q.shape, BF), jax.ShapeDtypeStruct((heads, tokens), F32)],
        scratch_shapes=[pltpu.VMEM((kb, bq), F32), pltpu.VMEM((kb, HEAD + 8, bq), F32)],
        compiler_params=_params("arbitrary", "arbitrary"),
        cost_estimate=pl.CostEstimate(flops=8 * heads * tokens * tokens * HEAD, transcendentals=heads * tokens * tokens, bytes_accessed=8 * tokens * cols),
        name="attend",
    )(q, k, v)


def _attend_bwd(q_ref, k_ref, v_ref, o_ref, do_ref, lse_ref, cq_ref, sq_ref, cos_ref, sin_ref, dq_ref, dk_ref, dv_ref, dq_s, dk_s, dv_s, *, kb, bq, scale):
    iq = pl.program_id(1)
    e = scale * LOG2E

    @pl.when(iq == 0)
    def _():
        dk_s[...] = jnp.zeros_like(dk_s)
        dv_s[...] = jnp.zeros_like(dv_s)

    dq_s[...] = jnp.zeros_like(dq_s)
    h0 = pl.program_id(0) * kb
    lses = [lse_ref[pl.ds(h0 + i, 1), :] * LOG2E for i in range(kb)]
    deltas = [(do_ref[:, _head(i)].astype(F32) * o_ref[:, _head(i)].astype(F32)).T.sum(axis=0, keepdims=True) for i in range(kb)]

    def block(j, masked):
        here = pl.ds(pl.multiple_of(j * bq, bq), bq)
        scores = [_dot(k_ref[here, _head(i)], q_ref[:, _head(i)], 1, 1) for i in range(kb)]
        dps = [_dot(v_ref[here, _head(i)], do_ref[:, _head(i)], 1, 1) for i in range(kb)]
        ok = _below(bq, bq) if masked else None
        for i in range(kb):
            p = jnp.exp2(scores[i] * e - lses[i])
            if masked:
                p = jnp.where(ok, p, 0.0)
            ds = (p * (dps[i] - deltas[i])).astype(BF)
            dv_s[i, here, :] += _dot(p.astype(BF), do_ref[:, _head(i)])
            dk_s[i, here, :] += _dot(ds, q_ref[:, _head(i)])
            dq_s[i] += _dot(k_ref[here, _head(i)].T, ds)

    lax.fori_loop(0, iq, lambda j, _: block(j, False), None)
    block(iq, True)
    for i in range(kb):
        d = (dq_s[i] * scale).T
        dq_ref[:, _head(i)] = (d * cq_ref[...] + pltpu.roll(d * sq_ref[...], HEAD // 2, 1)).astype(BF)

    @pl.when(iq == pl.num_programs(1) - 1)
    def _():
        for i in range(kb):
            def some(n, _):
                here = pl.ds(pl.multiple_of(n * bq, bq), bq)
                d = dk_s[i, here, :] * scale
                dk_ref[here, _head(i)] = (d * cos_ref[here, :] + pltpu.roll(d * sin_ref[here, :], HEAD // 2, 1)).astype(BF)
                dv_ref[here, _head(i)] = dv_s[i, here, :].astype(BF)

            lax.fori_loop(0, dk_ref.shape[0] // bq, some, None)


def attend_bwd(q, k, v, o, do, lse, cos, sin, kb=4, bq=512):
    tokens, cols = q.shape
    heads = cols // HEAD
    some = pl.BlockSpec((bq, kb * HEAD), lambda h, n: (n, h))
    keys = pl.BlockSpec((tokens, kb * HEAD), lambda h, n: (0, h))
    near = pl.BlockSpec((bq, HEAD), lambda h, n: (n, 0))
    whole = pl.BlockSpec((tokens, HEAD), lambda h, n: (0, 0))
    return pl.pallas_call(
        functools.partial(_attend_bwd, kb=kb, bq=bq, scale=HEAD**-0.5),
        grid=(heads // kb, tokens // bq),
        in_specs=[some, keys, keys, some, some, pl.BlockSpec((heads, bq), lambda h, n: (0, n)), near, near, whole, whole],
        out_specs=[some, keys, keys],
        out_shape=[jax.ShapeDtypeStruct(q.shape, BF)] * 3,
        scratch_shapes=[pltpu.VMEM((kb, HEAD, bq), F32), pltpu.VMEM((kb, tokens, HEAD), F32), pltpu.VMEM((kb, tokens, HEAD), F32)],
        compiler_params=_params("arbitrary", "arbitrary"),
        cost_estimate=pl.CostEstimate(flops=16 * heads * tokens * tokens * HEAD, transcendentals=heads * tokens * tokens, bytes_accessed=16 * tokens * cols),
        name="attend_bwd",
    )(q, k, v, o, do, lse, cos, sin, cos, sin)


def _mlp(b_ref, dy_ref, go, gr, uo, ur, dn_ref, *rest, rows, given, last):
    sums, rest = (rest[:5], rest[5:]) if given else (None, rest)
    db_ref, outs, (dg_s, du_s, dd_s, db_s) = rest[0], rest[1:6], rest[6:]
    n = pl.program_id(0)
    tokens, d = b_ref.shape
    half = d // 2

    @pl.when(n == 0)
    def _():
        db_s[...] = jnp.zeros_like(db_s)

    dg_s[...] = jnp.zeros_like(dg_s)
    du_s[...] = jnp.zeros_like(du_s)
    dd_s[...] = sums[4][...] if given else jnp.zeros_like(dd_s)
    gate = jnp.concatenate([go[...], gr[...]], axis=0)
    up = jnp.concatenate([uo[...], ur[...]], axis=0)
    gate_t, up_t, down = gate.T, up.T, dn_ref[...]

    def some(m, _):
        here = pl.ds(pl.multiple_of(m * rows, rows), rows)
        b, dy = b_ref[here, :], dy_ref[here, :]
        g = _dot(gate_t, b, 1, 1)
        u = _dot(up_t, b, 1, 1)
        dh = _dot(down, dy, 1, 1).astype(BF).astype(F32)
        s = jax.nn.sigmoid(g)
        silu = g * s
        hidden = (silu * u).astype(BF)
        du = (dh * silu).astype(BF)
        dg = (dh * u * (s + silu * (1 - s))).astype(BF)
        dd_s[...] += _dot(hidden, dy)
        dg_s[...] += _dot(dg, b)
        du_s[...] += _dot(du, b)
        db_s[:, here] += _dot(gate, dg) + _dot(up, du)

    lax.fori_loop(0, tokens // rows, some, None)
    for s, k in ((dg_s, 0), (du_s, 2)):
        t = s[...].T
        for part, o in ((t[:half], k), (t[half:], k + 1)):
            outs[o][...] = ((part + sums[o][...]) if given else part).astype(outs[o].dtype)
    outs[4][...] = dd_s[...].astype(outs[4].dtype)

    @pl.when(n == pl.num_programs(0) - 1)
    def _():
        db_ref[...] = db_s[...].T.astype(BF)


def mlp(b, dy, gate, up, down, sums=None, units=512, rows=512):
    tokens, d = b.shape
    hidden = down.shape[0]
    kind = BF if sums is not None else F32
    given = list(sums) if sums is not None else []
    whole = pl.BlockSpec((tokens, d), lambda n: (0, 0))
    w = pl.BlockSpec((d // 2, units), lambda n: (0, n))
    wd = pl.BlockSpec((units, d), lambda n: (n, 0))
    db, *dw = pl.pallas_call(
        functools.partial(_mlp, rows=rows, given=sums is not None, last=sums is not None),
        grid=(hidden // units,),
        in_specs=[whole, whole, w, w, w, w, wd, *([w, w, w, w, wd] if given else [])],
        out_specs=[whole, w, w, w, w, wd],
        out_shape=[jax.ShapeDtypeStruct((tokens, d), BF), *[jax.ShapeDtypeStruct((d // 2, hidden), kind)] * 4, jax.ShapeDtypeStruct((hidden, d), kind)],
        scratch_shapes=[pltpu.VMEM((units, d), F32)] * 3 + [pltpu.VMEM((d, tokens), F32)],
        compiler_params=_params("arbitrary"),
        cost_estimate=pl.CostEstimate(flops=16 * tokens * d * hidden, transcendentals=tokens * hidden, bytes_accessed=30 * d * hidden),
        name="mlp",
    )(b, dy, *gate, *up, down, *given)
    return db, dw


def _proj_bwd(a_ref, dq_ref, dk_ref, dv_ref, qo, qr, ko, kr, vo, vr, *rest, given):
    sums, rest = (rest[:6], rest[6:]) if given else (None, rest)
    da_ref, outs, accs = rest[0], rest[1:7], rest[7:]
    n = pl.program_id(0)
    half = a_ref.shape[1] // 2

    @pl.when(n == 0)
    def _():
        for i, s in enumerate(accs):
            s[...] = jnp.concatenate([sums[2 * i][...], sums[2 * i + 1][...]], axis=0) if given else jnp.zeros_like(s)

    a_t = a_ref[...].T
    ds = (dq_ref[...], dk_ref[...], dv_ref[...])
    da_ref[:, :half] = (_dot(ds[0], qo[...], 1, 1) + _dot(ds[1], ko[...], 1, 1) + _dot(ds[2], vo[...], 1, 1)).astype(BF)
    da_ref[:, half:] = (_dot(ds[0], qr[...], 1, 1) + _dot(ds[1], kr[...], 1, 1) + _dot(ds[2], vr[...], 1, 1)).astype(BF)
    for i, s in enumerate(accs):
        s[...] += _dot(a_t, ds[i])

    @pl.when(n == pl.num_programs(0) - 1)
    def _():
        for i, s in enumerate(accs):
            outs[2 * i][...] = s[:half, :].astype(outs[0].dtype)
            outs[2 * i + 1][...] = s[half:, :].astype(outs[0].dtype)


def proj_bwd(a, ds, ws, sums=None, rows=512):
    tokens, d = a.shape
    cols = ds[0].shape[1]
    kind = BF if sums is not None else F32
    given = list(sums) if sums is not None else []
    some = lambda wide: pl.BlockSpec((rows, wide), lambda n: (n, 0))
    w = pl.BlockSpec((d // 2, cols), lambda n: (0, 0))
    da, *dw = pl.pallas_call(
        functools.partial(_proj_bwd, given=sums is not None),
        grid=(tokens // rows,),
        in_specs=[some(d), *[some(cols)] * 3, *[w] * 6, *[w] * len(given)],
        out_specs=[some(d), *[w] * 6],
        out_shape=[jax.ShapeDtypeStruct((tokens, d), BF), *[jax.ShapeDtypeStruct((d // 2, cols), kind)] * 6],
        scratch_shapes=[pltpu.VMEM((d, cols), F32)] * 3,
        compiler_params=_params("arbitrary"),
        cost_estimate=pl.CostEstimate(flops=12 * tokens * d * cols, transcendentals=0, bytes_accessed=2 * (2 * tokens * d + 9 * d * cols + 3 * tokens * cols)),
        name="proj_bwd",
    )(a, *ds, *ws, *given)
    return da, dw


def normed(h):
    wide = h.astype(F32)
    scale = lax.rsqrt(jnp.mean(wide**2, -1, keepdims=True) + 1e-6)
    return (wide * scale).astype(BF)


def tables(tokens):
    half = HEAD // 2
    angle = jnp.arange(tokens, dtype=F32)[:, None] * THETA ** (-jnp.arange(half, dtype=F32) / half)
    cos, sin = jnp.cos(angle), jnp.sin(angle)
    return jnp.concatenate([cos, cos], 1), jnp.concatenate([-sin, sin], 1)


def solution(mesh):
    swap = [(0, 1), (1, 0)]
    tp = mesh.shape["tp"]

    def step(x, dy, wq, wk, wv, wo, wg, wu, wd):
        x, dy = x[0], dy[0]
        p = lax.axis_index("dp")
        d = x.shape[1]

        def rel(t):
            return jnp.where(p == 0, t, jnp.roll(t, d // 2, 1))

        def fetch(w):
            half = w.shape[1] // 2
            own, other = (lax.dynamic_slice_in_dim(w, n * half, half, 1) for n in (p, 1 - p))
            return own, lax.ppermute(other, "dp", swap)

        def give(own, other):
            got = lax.ppermute(other, "dp", swap)
            return jnp.where(p == 0, jnp.concatenate([own, got], 1), jnp.concatenate([got, own], 1))

        def gather(t):
            return lax.all_gather(t, "tp", axis=0, tiled=True)

        def both(t, turn):
            other = lax.ppermute(t, "dp", swap)
            return [gather(turn(jnp.where(p == s, t, other))) for s in (0, 1)]

        def spread(t, s, turn):
            other = lax.ppermute(t, "dp", [(s, 1 - s)])
            return gather(turn(jnp.where(p == s, t, other)))

        def collect(part, s, turn):
            mine = turn(lax.psum_scatter(part, "tp", scatter_dimension=0, tiled=True))
            return mine.astype(F32) + lax.ppermute(mine, "dp", [(1 - s, s)]).astype(F32)

        same = lambda t: t
        n1, back1 = jax.vjp(normed, x)
        a = both(n1, rel)
        ws = [w for pair in map(fetch, (wq, wk, wv)) for w in pair]
        gate, up = fetch(wg), fetch(wu)
        dys = both(dy, same)
        cos, sin = tables(tp * x.shape[0])

        kept, h, b = [], [], []
        for s in (0, 1):
            q, k, v = qkv(a[s], ws, cos, sin)
            o, lse = attend(q, k, v)
            kept.append((q, k, v, o, lse))
            part = _dot(o, wo).astype(BF)
            h.append((x.astype(F32) + collect(part, s, same)).astype(BF))
            b.append(spread(normed(h[s]), s, rel))
        sums, dh, d_all = None, [], []
        for s in (0, 1):
            db, sums = mlp(b[s], dys[s], gate, up, wd, sums)
            n, back2 = jax.vjp(normed, h[s])
            dh.append((dy.astype(F32) + back2(collect(db, s, rel).astype(BF))[0].astype(F32)).astype(BF))
            d_all.append(spread(dh[s], s, same))
        dwg, dwu, dwd = give(*sums[:2]), give(*sums[2:4]), sums[4]
        dwo = (_dot(kept[0][3], d_all[0], 0, 0) + _dot(kept[1][3], d_all[1], 0, 0)).astype(BF)
        sums, dx = None, []
        for s in (0, 1):
            q, k, v, o, lse = kept[s]
            do = _dot(d_all[s], wo, 1, 1).astype(BF)
            ds = attend_bwd(q, k, v, o, do, lse, cos, sin)
            da, sums = proj_bwd(a[s], ds, ws, sums)
            dx.append((dh[s].astype(F32) + back1(collect(da, s, rel).astype(BF))[0].astype(F32)).astype(BF))
        dw = [give(*sums[2 * i : 2 * i + 2]) for i in range(3)]
        return (jnp.where(p == 0, dx[0], dx[1])[None], *dw, dwo, dwg, dwu, dwd)

    states, by_columns, by_rows = P("dp", "tp", None), P("dp", "tp"), P(("tp", "dp"), None)
    weights = (by_columns, by_columns, by_columns, by_rows, by_columns, by_columns, by_rows)
    return jax.shard_map(step, mesh=mesh, in_specs=(states, states, *weights), out_specs=(states, *weights), check_vma=False)
```

```python
import functools

import jax
import jax.numpy as jnp
from jax import lax
from jax.experimental import pallas as pl
from jax.experimental.pallas import tpu as pltpu
from jax.sharding import PartitionSpec as P

HEAD = 128
THETA = 10000
NEG = -1e30
HIDDEN = 2 * NEG
LOG2E = 1.4426950408889634
VMEM = 60 * 2**20
BF, F32 = jnp.bfloat16, jnp.float32


def _dot(a, b, ca=1, cb=0):
    return lax.dot_general(a, b, (((ca,), (cb,)), ((), ())), preferred_element_type=F32)


def _params(*kinds):
    return pltpu.CompilerParams(dimension_semantics=kinds, vmem_limit_bytes=VMEM)


def _head(i):
    return slice(i * HEAD, (i + 1) * HEAD)


def _whole(scratch, own, other, place):
    half = own.shape[0]
    scratch[pl.ds(pl.multiple_of(place * half, half), half), :] = own
    scratch[pl.ds(pl.multiple_of((1 - place) * half, half), half), :] = other


def _qkv(place_ref, a_ref, qo, ko, vo, qr, kr, vr, cos_ref, sin_ref, q_ref, k_ref, v_ref, w_s, *, rows):
    wide = qo.shape[1]
    for i, (own, other) in enumerate(((qo, qr), (ko, kr), (vo, vr))):
        _whole(w_s.at[:, i * wide : (i + 1) * wide], own[...], other[...], place_ref[0])

    def some(n, _):
        here = pl.ds(pl.multiple_of(n * rows, rows), rows)
        t = _dot(a_ref[here, :], w_s[...]).astype(BF)
        cos, sin = cos_ref[here, :], sin_ref[here, :]
        for i, out in enumerate((q_ref, k_ref, v_ref)):
            for h in range(wide // HEAD):
                u = t[:, i * wide + h * HEAD : i * wide + (h + 1) * HEAD]
                if i < 2:
                    u = u.astype(F32)
                    u = (u * cos + pltpu.roll(u, HEAD // 2, 1) * sin).astype(BF)
                out[here, _head(h)] = u

    lax.fori_loop(0, a_ref.shape[0] // rows, some, None)


def qkv(place, a, own, other, cos, sin, wide=256, rows=512):
    tokens, d = a.shape
    cols = other.shape[1] // 3
    steps = cols // wide
    whole = lambda *shape: pl.BlockSpec(shape, lambda n, p: (0, 0))
    mine = pl.BlockSpec((d // 2, wide), lambda n, p: (0, p[0] * steps + n))
    got = [pl.BlockSpec((d // 2, wide), functools.partial(lambda i, n, p: (0, i * steps + n), i)) for i in range(3)]
    out = pl.BlockSpec((tokens, wide), lambda n, p: (0, n))
    return pl.pallas_call(
        functools.partial(_qkv, rows=rows),
        grid_spec=pltpu.PrefetchScalarGridSpec(
            num_scalar_prefetch=1,
            grid=(steps,),
            in_specs=[whole(tokens, d), *[mine] * 3, *got, whole(tokens, HEAD), whole(tokens, HEAD)],
            out_specs=[out] * 3,
            scratch_shapes=[pltpu.VMEM((d, 3 * wide), BF)],
        ),
        out_shape=[jax.ShapeDtypeStruct((tokens, cols), BF)] * 3,
        compiler_params=_params("arbitrary"),
        cost_estimate=pl.CostEstimate(flops=6 * tokens * d * cols, transcendentals=0, bytes_accessed=2 * (tokens * d + 3 * d * cols + 3 * tokens * cols)),
        name="qkv",
    )(place, a, *own, other, other, other, cos, sin)


def _below(bk, bq):
    return lax.broadcasted_iota(jnp.int32, (bk, bq), 1) >= lax.broadcasted_iota(jnp.int32, (bk, bq), 0)


def _attend(q_ref, k_ref, v_ref, o_ref, lse_ref, top_s, mix_s, *, kb, bq, scale):
    iq = pl.program_id(1)
    e = scale * LOG2E
    top_s[...] = jnp.full(top_s.shape, NEG, F32)
    mix_s[...] = jnp.zeros(mix_s.shape, F32)
    ones = jnp.ones((8, bq), BF)

    def block(j, masked):
        here = pl.ds(pl.multiple_of(j * bq, bq), bq)
        scores = [_dot(k_ref[here, _head(i)], q_ref[:, _head(i)], 1, 1) for i in range(kb)]
        ok = _below(bq, bq) if masked else None
        weights, keeps = [], []
        for i, s in enumerate(scores):
            if masked:
                s = jnp.where(ok, s, HIDDEN)
            old = top_s[i : i + 1, :]
            top = jnp.maximum(old, s.max(axis=0, keepdims=True))
            top_s[i : i + 1, :] = top
            weights.append(jnp.exp2((s - top) * e).astype(BF))
            keeps.append(jnp.exp2((old - top) * e))
        for i in range(kb):
            values = jnp.concatenate([v_ref[here, _head(i)].T, ones], axis=0)
            mix_s[i] = mix_s[i] * keeps[i] + _dot(values, weights[i])

    lax.fori_loop(0, iq, lambda j, _: block(j, False), None)
    block(iq, True)
    for i in range(kb):
        top, total = top_s[i : i + 1, :], mix_s[i, HEAD : HEAD + 1, :]
        o_ref[:, _head(i)] = (mix_s[i, :HEAD, :] * (1 / total)).T.astype(BF)
        lse_ref[0, i : i + 1, :] = top * scale + jnp.log(total)


def attend(q, k, v, part=0, parts=1, before=None, kb=4, bq=512):
    tokens, cols = q.shape
    heads = cols // HEAD
    groups = heads // kb // parts
    at = part * groups
    some = pl.BlockSpec((bq, kb * HEAD), lambda h, n: (n, at + h))
    keys = pl.BlockSpec((tokens, kb * HEAD), lambda h, n: (0, at + h))
    given = [] if before is None else list(before)

    def kernel(q_ref, k_ref, v_ref, *rest):
        _attend(q_ref, k_ref, v_ref, *rest[len(given) :], kb=kb, bq=bq, scale=HEAD**-0.5)

    return pl.pallas_call(
        kernel,
        grid=(groups, tokens // bq),
        in_specs=[some, keys, keys, *[pl.BlockSpec(memory_space=pl.ANY)] * len(given)],
        out_specs=[some, pl.BlockSpec((1, kb, bq), lambda h, n: (at + h, 0, n))],
        out_shape=[jax.ShapeDtypeStruct(q.shape, BF), jax.ShapeDtypeStruct((heads // kb, kb, tokens), F32)],
        scratch_shapes=[pltpu.VMEM((kb, bq), F32), pltpu.VMEM((kb, HEAD + 8, bq), F32)],
        input_output_aliases={3 + i: i for i in range(len(given))},
        compiler_params=_params("arbitrary", "arbitrary"),
        cost_estimate=pl.CostEstimate(flops=8 * heads // parts * tokens * tokens * HEAD, transcendentals=heads // parts * tokens * tokens, bytes_accessed=8 * tokens * cols // parts),
        name="attend",
    )(q, k, v, *given)


def _attend_bwd(q_ref, k_ref, v_ref, o_ref, do_ref, lse_ref, cq_ref, sq_ref, cos_ref, sin_ref, dq_ref, dk_ref, dv_ref, dq_s, dk_s, dv_s, *, kb, bq, scale):
    iq = pl.program_id(1)
    e = scale * LOG2E

    @pl.when(iq == 0)
    def _():
        dk_s[...] = jnp.zeros_like(dk_s)
        dv_s[...] = jnp.zeros_like(dv_s)

    dq_s[...] = jnp.zeros_like(dq_s)
    lses = [lse_ref[0, i : i + 1, :] * LOG2E for i in range(kb)]
    deltas = [(do_ref[:, _head(i)].astype(F32) * o_ref[:, _head(i)].astype(F32)).T.sum(axis=0, keepdims=True) for i in range(kb)]

    def block(j, masked):
        here = pl.ds(pl.multiple_of(j * bq, bq), bq)
        scores = [_dot(k_ref[here, _head(i)], q_ref[:, _head(i)], 1, 1) for i in range(kb)]
        dps = [_dot(v_ref[here, _head(i)], do_ref[:, _head(i)], 1, 1) for i in range(kb)]
        ok = _below(bq, bq) if masked else None
        for i in range(kb):
            p = jnp.exp2(scores[i] * e - lses[i])
            if masked:
                p = jnp.where(ok, p, 0.0)
            ds = (p * (dps[i] - deltas[i])).astype(BF)
            dv_s[i, here, :] += _dot(p.astype(BF), do_ref[:, _head(i)])
            dk_s[i, here, :] += _dot(ds, q_ref[:, _head(i)])
            dq_s[i] += _dot(k_ref[here, _head(i)].T, ds)

    lax.fori_loop(0, iq, lambda j, _: block(j, False), None)
    block(iq, True)
    for i in range(kb):
        d = (dq_s[i] * scale).T
        dq_ref[:, _head(i)] = (d * cq_ref[...] + pltpu.roll(d * sq_ref[...], HEAD // 2, 1)).astype(BF)

    @pl.when(iq == pl.num_programs(1) - 1)
    def _():
        for i in range(kb):
            def some(n, _):
                here = pl.ds(pl.multiple_of(n * bq, bq), bq)
                d = dk_s[i, here, :] * scale
                dk_ref[here, _head(i)] = (d * cos_ref[here, :] + pltpu.roll(d * sin_ref[here, :], HEAD // 2, 1)).astype(BF)
                dv_ref[here, _head(i)] = dv_s[i, here, :].astype(BF)

            lax.fori_loop(0, dk_ref.shape[0] // bq, some, None)


def attend_bwd(q, k, v, o, do, lse, cos, sin, part=0, parts=1, before=None, bq=512):
    tokens, cols = q.shape
    kb = lse.shape[1]
    heads = cols // HEAD
    groups = heads // kb // parts
    at = part * groups
    some = pl.BlockSpec((bq, kb * HEAD), lambda h, n: (n, at + h))
    keys = pl.BlockSpec((tokens, kb * HEAD), lambda h, n: (0, at + h))
    near = pl.BlockSpec((bq, HEAD), lambda h, n: (n, 0))
    whole = pl.BlockSpec((tokens, HEAD), lambda h, n: (0, 0))
    given = [] if before is None else list(before)

    def kernel(*refs):
        _attend_bwd(*refs[:10], *refs[10 + len(given) :], kb=kb, bq=bq, scale=HEAD**-0.5)

    return pl.pallas_call(
        kernel,
        grid=(groups, tokens // bq),
        in_specs=[some, keys, keys, some, some, pl.BlockSpec((1, kb, bq), lambda h, n: (at + h, 0, n)), near, near, whole, whole,
                  *[pl.BlockSpec(memory_space=pl.ANY)] * len(given)],
        out_specs=[some, keys, keys],
        out_shape=[jax.ShapeDtypeStruct(q.shape, BF)] * 3,
        scratch_shapes=[pltpu.VMEM((kb, HEAD, bq), F32), pltpu.VMEM((kb, tokens, HEAD), F32), pltpu.VMEM((kb, tokens, HEAD), F32)],
        input_output_aliases={10 + i: i for i in range(len(given))},
        compiler_params=_params("arbitrary", "arbitrary"),
        cost_estimate=pl.CostEstimate(flops=16 * heads // parts * tokens * tokens * HEAD, transcendentals=heads // parts * tokens * tokens, bytes_accessed=16 * tokens * cols // parts),
        name="attend_bwd",
    )(q, k, v, o, do, lse, cos, sin, cos, sin, *given)


def _mlp(place_ref, b_ref, dy_ref, go, uo, gr, ur, dn_ref, *rest, rows, given, begun):
    sums, rest = (rest[:4], rest[4:]) if given else (None, rest)
    db_in, rest = (rest[0], rest[1:]) if begun else (None, rest)
    db_ref, dg_ref, du_ref, dother_ref, dd_ref, gate_s, up_s, dg_s, du_s, dd_s, db_s = rest
    n, place = pl.program_id(0), place_ref[0]
    tokens, d = b_ref.shape
    half = d // 2
    mine, theirs = pl.ds(pl.multiple_of(place * half, half), half), pl.ds(pl.multiple_of((1 - place) * half, half), half)

    @pl.when(n == 0)
    def _():
        db_s[...] = db_in[...] if begun else jnp.zeros_like(db_s)

    dg_s[...] = jnp.zeros_like(dg_s)
    du_s[...] = jnp.zeros_like(du_s)
    dd_s[...] = sums[3][...] if given else jnp.zeros_like(dd_s)
    _whole(gate_s, go[...], gr[...], place)
    _whole(up_s, uo[...], ur[...], place)
    gate_t, up_t = gate_s[...].T, up_s[...].T

    def some(m, _):
        here = pl.ds(pl.multiple_of(m * rows, rows), rows)
        b, dy = b_ref[here, :], dy_ref[here, :]
        g = _dot(gate_t, b, 1, 1)
        u = _dot(up_t, b, 1, 1)
        dh = _dot(dn_ref[...], dy, 1, 1).astype(BF).astype(F32)
        s = jax.nn.sigmoid(g)
        silu = g * s
        hidden = (silu * u).astype(BF)
        du = (dh * silu).astype(BF)
        dg = (dh * u * (s + silu * (1 - s))).astype(BF)
        dd_s[...] += _dot(hidden, dy)
        dg_s[...] += _dot(dg, b)
        du_s[...] += _dot(du, b)
        db_s[:, here] += _dot(gate_s[...], dg) + _dot(up_s[...], du)

    lax.fori_loop(0, tokens // rows, some, None)
    for i, (s, out, turned) in enumerate(((dg_s, dg_ref, gate_s), (du_s, du_ref, up_s))):
        del turned
        t = s[...].T
        s_own = jnp.where(place == 0, t[:half], t[half:])
        s_other = jnp.where(place == 0, t[half:], t[:half])
        out[...] = ((s_own + sums[i][...]) if given else s_own).astype(out.dtype)
        dother_ref[i] = ((s_other + sums[2][i]) if given else s_other).astype(dother_ref.dtype)
    dd_ref[...] = dd_s[...].astype(dd_ref.dtype)

    @pl.when(n == pl.num_programs(0) - 1)
    def _():
        db_ref[...] = db_s[...].T.astype(BF) if begun else db_s[...]


def mlp(place, b, dy, gate, up, other, down, part, sums=None, db=None, units=512, rows=512):
    tokens, d = b.shape
    hidden = down.shape[0] // 2
    steps = hidden // units
    kind = BF if sums is not None else F32
    given = [*(sums or []), *([db] if db is not None else [])]
    whole = pl.BlockSpec((tokens, d), lambda n, p: (0, 0))
    whole_t = pl.BlockSpec((d, tokens), lambda n, p: (0, 0))
    own = pl.BlockSpec((d // 2, units), lambda n, p: (0, (2 * p[0] + part) * steps + n))
    got = [pl.BlockSpec((d // 2, units), functools.partial(lambda i, n, p: (0, (2 * i + part) * steps + n), i)) for i in range(2)]
    w = pl.BlockSpec((d // 2, units), lambda n, p: (0, n))
    w2 = pl.BlockSpec((2, d // 2, units), lambda n, p: (0, 0, n))
    wd = pl.BlockSpec((units, d), lambda n, p: (n, 0))
    wd_in = pl.BlockSpec((units, d), lambda n, p: (part * steps + n, 0))
    shape = jax.ShapeDtypeStruct
    out, *dw = pl.pallas_call(
        functools.partial(_mlp, rows=rows, given=sums is not None, begun=db is not None),
        grid_spec=pltpu.PrefetchScalarGridSpec(
            num_scalar_prefetch=1,
            grid=(steps,),
            in_specs=[whole, whole, own, own, *got, wd_in, *([w, w, w2, wd] if sums is not None else []), *([whole_t] if db is not None else [])],
            out_specs=[whole if db is not None else whole_t, w, w, w2, wd],
            scratch_shapes=[pltpu.VMEM((d, units), BF)] * 2 + [pltpu.VMEM((units, d), F32)] * 3 + [pltpu.VMEM((d, tokens), F32)],
        ),
        out_shape=[shape((tokens, d), BF) if db is not None else shape((d, tokens), F32), shape((d // 2, hidden), kind), shape((d // 2, hidden), kind),
                   shape((2, d // 2, hidden), kind), shape((hidden, d), kind)],
        compiler_params=_params("arbitrary"),
        cost_estimate=pl.CostEstimate(flops=16 * tokens * d * hidden, transcendentals=tokens * hidden, bytes_accessed=30 * d * hidden),
        name="mlp",
    )(place, b, dy, gate, up, other, other, down, *given)
    return out, dw


def _proj_bwd(place_ref, a_ref, dq_ref, dk_ref, dv_ref, qo, ko, vo, other, *rest, given):
    sums, rest = (rest[:4], rest[4:]) if given else (None, rest)
    da_ref, outs, dother_ref, w_s, accs = rest[0], rest[1:4], rest[4], rest[5], rest[6:]
    n, place = pl.program_id(0), place_ref[0]
    half = a_ref.shape[1] // 2
    cols = qo.shape[1]
    mine, theirs = pl.ds(pl.multiple_of(place * half, half), half), pl.ds(pl.multiple_of((1 - place) * half, half), half)
    part = [slice(i * cols, (i + 1) * cols) for i in range(3)]

    @pl.when(n == 0)
    def _():
        for i, (s, own) in enumerate(zip(accs, (qo, ko, vo))):
            _whole(w_s.at[:, part[i]], own[...], other[:, part[i]], place)
            if given:
                s[mine, :] = sums[i][...]
                s[theirs, :] = sums[3][:, part[i]]
            else:
                s[...] = jnp.zeros_like(s)

    a_t = a_ref[...].T
    ds = (dq_ref[...], dk_ref[...], dv_ref[...])
    da_ref[...] = sum(_dot(ds[i], w_s[:, part[i]], 1, 1) for i in range(3)).astype(BF)
    for i, s in enumerate(accs):
        s[...] += _dot(a_t, ds[i])

    @pl.when(n == pl.num_programs(0) - 1)
    def _():
        for i, s in enumerate(accs):
            outs[i][...] = s[mine, :].astype(outs[i].dtype)
            dother_ref[:, part[i]] = s[theirs, :].astype(dother_ref.dtype)


def proj_bwd(place, a, ds, own, other, sums=None, rows=512):
    tokens, d = a.shape
    cols = ds[0].shape[1]
    kind = BF if sums is not None else F32
    given = list(sums) if sums is not None else []
    some = lambda wide: pl.BlockSpec((rows, wide), lambda n, p: (n, 0))
    mine = pl.BlockSpec((d // 2, cols), lambda n, p: (0, p[0]))
    w = pl.BlockSpec((d // 2, cols), lambda n, p: (0, 0))
    w3 = pl.BlockSpec((d // 2, 3 * cols), lambda n, p: (0, 0))
    shape = jax.ShapeDtypeStruct
    da, *dw = pl.pallas_call(
        functools.partial(_proj_bwd, given=sums is not None),
        grid_spec=pltpu.PrefetchScalarGridSpec(
            num_scalar_prefetch=1,
            grid=(tokens // rows,),
            in_specs=[some(d), *[some(cols)] * 3, *[mine] * 3, w3, *([w, w, w, w3] if given else [])],
            out_specs=[some(d), w, w, w, w3],
            scratch_shapes=[pltpu.VMEM((d, 3 * cols), BF)] + [pltpu.VMEM((d, cols), F32)] * 3,
        ),
        out_shape=[shape((tokens, d), BF), *[shape((d // 2, cols), kind)] * 3, shape((d // 2, 3 * cols), kind)],
        compiler_params=_params("arbitrary"),
        cost_estimate=pl.CostEstimate(flops=12 * tokens * d * cols, transcendentals=0, bytes_accessed=2 * (2 * tokens * d + 9 * d * cols + 3 * tokens * cols)),
        name="proj_bwd",
    )(place, a, *ds, *own, other, *given)
    return da, dw


def normed(h):
    wide = h.astype(F32)
    scale = lax.rsqrt(jnp.mean(wide**2, -1, keepdims=True) + 1e-6)
    return (wide * scale).astype(BF)


def tables(tokens):
    half = HEAD // 2
    angle = jnp.arange(tokens, dtype=F32)[:, None] * THETA ** (-jnp.arange(half, dtype=F32) / half)
    cos, sin = jnp.cos(angle), jnp.sin(angle)
    return jnp.concatenate([cos, cos], 1), jnp.concatenate([-sin, sin], 1)


def after(t, *those):
    return lax.optimization_barrier((t, *those))[0]


def solution(mesh):
    swap = [(0, 1), (1, 0)]
    everyone = ("tp", "dp")

    def step(x, dy, wq, wk, wv, wo, wg, wu, wd):
        p = lax.axis_index("dp")
        place = p.astype(jnp.int32)[None]
        x, dy = x[0], dy[0]
        tokens = x.shape[0] * mesh.shape["tp"]

        def halves(t, axis, n):
            size = t.shape[axis] // 2
            return lax.dynamic_slice_in_dim(t, n * size, size, axis)

        def by_place(mine, theirs):
            return jnp.where(p == 0, mine, theirs), jnp.where(p == 0, theirs, mine)

        def runs(t, those):
            return by_place(halves(t, 0, p), after(lax.ppermute(halves(t, 0, 1 - p), "dp", swap), those))

        def gather(t):
            return lax.all_gather(t, everyone, axis=0, tiled=True)

        def collect(part):
            return lax.psum_scatter(part, everyone, scatter_dimension=0, tiled=True)

        def plus(t, more):
            return (t.astype(F32) + more.astype(F32)).astype(BF)

        send = jnp.concatenate([halves(w, 1, 1 - p) for w in (wq, wk, wv)], 1)
        send2 = jnp.concatenate([halves(w, 1, 1 - p) for w in (wg, wu)], 1)
        xs = runs(x, send)
        other = lax.ppermute(send, "dp", swap)
        other2 = lax.ppermute(send2, "dp", swap)
        dys = runs(dy, send2)
        norms, backs = zip(*(jax.vjp(normed, t) for t in xs))
        a = [gather(t) for t in norms]
        dy_all = [gather(t) for t in dys]
        cos, sin = tables(tokens)
        own = (wq, wk, wv)

        def project(o):
            return _dot(o, wo).astype(BF)

        q0 = qkv(place, after(a[0], *dys), own, other, cos, sin)
        o0 = attend(*q0)
        h0 = collect(project(o0[0]))
        q1 = qkv(place, after(a[1], o0[0]), own, other, cos, sin)
        o1 = attend(*q1, 0, 2)
        h0 = plus(xs[0], after(h0, o1[0]))
        b0, back0 = jax.vjp(normed, h0)
        o1 = attend(after(q1[0], b0), *q1[1:], 1, 2, o1)
        b0 = gather(b0)
        h1 = collect(project(o1[0]))
        db0, w0a = mlp(place, b0, dy_all[0], wg, wu, other2, wd, 0)
        h1 = plus(xs[1], after(h1, db0))
        b1, back1 = jax.vjp(normed, h1)
        db0, w0b = mlp(place, after(b0, b1), dy_all[0], wg, wu, other2, wd, 1, None, db0)
        b1 = gather(b1)
        db0 = collect(db0)
        db1, wa = mlp(place, b1, dy_all[1], wg, wu, other2, wd, 0, w0a)
        ga = lax.ppermute(wa[2], "dp", swap)
        dh0 = plus(dys[0], back0(after(db0, db1))[0])
        db1, wb = mlp(place, after(b1, dh0), dy_all[1], wg, wu, other2, wd, 1, w0b, db1)
        d0 = gather(dh0)
        gb = lax.ppermute(wb[2], "dp", swap)
        db1 = collect(db1)
        do0 = _dot(d0, wo, 1, 1).astype(BF)
        ds = attend_bwd(*q0, o0[0], do0, o0[1], cos, sin, 0, 2)
        dh1 = plus(dys[1], back1(after(db1, ds[0]))[0])
        ds = attend_bwd(after(q0[0], dh1), *q0[1:], o0[0], do0, o0[1], cos, sin, 1, 2, ds)
        d1 = gather(dh1)
        da0, sums = proj_bwd(place, a[0], ds, own, other)
        da0 = collect(da0)
        ds = attend_bwd(*q1, o1[0], _dot(d1, wo, 1, 1).astype(BF), o1[1], cos, sin)
        da1, sums = proj_bwd(place, a[1], ds, own, other, sums)
        gq = lax.ppermute(sums[3], "dp", swap)
        da1 = collect(da1)
        dx0 = plus(dh0, backs[0](da0)[0])
        dx1 = plus(dh1, backs[1](da1)[0])
        mine, theirs = by_place(dx0, dx1)
        theirs = lax.ppermute(theirs, "dp", swap)
        dx = jnp.concatenate(by_place(mine, theirs), 0)
        dwo = (_dot(o0[0], d0, 0, 0) + _dot(o1[0], d1, 0, 0)).astype(BF)

        def whole(mine, theirs):
            return jnp.where(p == 0, jnp.concatenate([*mine, *theirs], 1), jnp.concatenate([*theirs, *mine], 1))

        cols = sums[0].shape[1]
        dw = [whole([sums[i]], [gq[:, i * cols : (i + 1) * cols]]) for i in range(3)]
        dwg, dwu = (whole([wa[i], wb[i]], [ga[i], gb[i]]) for i in range(2))
        return (dx[None], *dw, dwo, dwg, dwu, jnp.concatenate([wa[3], wb[3]], 0))

    states, by_columns, by_rows = P("dp", "tp", None), P("dp", "tp"), P(("tp", "dp"), None)
    weights = (by_columns, by_columns, by_columns, by_rows, by_columns, by_columns, by_rows)
    return jax.shard_map(step, mesh=mesh, in_specs=(states, states, *weights), out_specs=(states, *weights), check_vma=False)
```

```python
import functools

import jax
import jax.numpy as jnp
from jax import lax
from jax.experimental import pallas as pl
from jax.experimental.pallas import tpu as pltpu
from jax.sharding import PartitionSpec as P

HEAD = 128
THETA = 10000
NEG = -1e30
HIDDEN = 2 * NEG
LOG2E = 1.4426950408889634
VMEM = 60 * 2**20
BF, F32 = jnp.bfloat16, jnp.float32


def _dot(a, b, ca=1, cb=0):
    return lax.dot_general(a, b, (((ca,), (cb,)), ((), ())), preferred_element_type=F32)


def _params(*kinds):
    return pltpu.CompilerParams(dimension_semantics=kinds, vmem_limit_bytes=VMEM)


def _head(i):
    return slice(i * HEAD, (i + 1) * HEAD)


def _whole(scratch, own, other, place):
    half = own.shape[0]
    scratch[pl.ds(pl.multiple_of(place * half, half), half), :] = own
    scratch[pl.ds(pl.multiple_of((1 - place) * half, half), half), :] = other


def _qkv(place_ref, a_ref, qo, ko, vo, qr, kr, vr, cos_ref, sin_ref, q_ref, k_ref, v_ref, w_s, *, rows):
    wide = qo.shape[1]
    for i, (own, other) in enumerate(((qo, qr), (ko, kr), (vo, vr))):
        _whole(w_s.at[:, i * wide : (i + 1) * wide], own[...], other[...], place_ref[0])

    def some(n, _):
        here = pl.ds(pl.multiple_of(n * rows, rows), rows)
        t = _dot(a_ref[here, :], w_s[...]).astype(BF)
        cos, sin = cos_ref[here, :], sin_ref[here, :]
        for i, out in enumerate((q_ref, k_ref, v_ref)):
            for h in range(wide // HEAD):
                u = t[:, i * wide + h * HEAD : i * wide + (h + 1) * HEAD]
                if i < 2:
                    u = u.astype(F32)
                    u = (u * cos + pltpu.roll(u, HEAD // 2, 1) * sin).astype(BF)
                out[here, _head(h)] = u

    lax.fori_loop(0, a_ref.shape[0] // rows, some, None)


def qkv(place, a, own, other, cos, sin, part, wide=256, rows=512):
    tokens, d = a.shape
    cols = other.shape[1] // 3
    steps = cols // wide
    whole = lambda *shape: pl.BlockSpec(shape, lambda n, p: (0, 0))
    mine = pl.BlockSpec((d // 2, wide), lambda n, p: (0, (2 * p[0] + part) * steps + n))
    got = [pl.BlockSpec((d // 2, wide), functools.partial(lambda i, n, p: (0, i * steps + n), i)) for i in range(3)]
    out = pl.BlockSpec((tokens, wide), lambda n, p: (0, n))
    return pl.pallas_call(
        functools.partial(_qkv, rows=rows),
        grid_spec=pltpu.PrefetchScalarGridSpec(
            num_scalar_prefetch=1,
            grid=(steps,),
            in_specs=[whole(tokens, d), *[mine] * 3, *got, whole(tokens, HEAD), whole(tokens, HEAD)],
            out_specs=[out] * 3,
            scratch_shapes=[pltpu.VMEM((d, 3 * wide), BF)],
        ),
        out_shape=[jax.ShapeDtypeStruct((tokens, cols), BF)] * 3,
        compiler_params=_params("arbitrary"),
        cost_estimate=pl.CostEstimate(flops=6 * tokens * d * cols, transcendentals=0, bytes_accessed=2 * (tokens * d + 3 * d * cols + 3 * tokens * cols)),
        name="qkv",
    )(place, a, *own, other, other, other, cos, sin)


def _below(bk, bq):
    return lax.broadcasted_iota(jnp.int32, (bk, bq), 1) >= lax.broadcasted_iota(jnp.int32, (bk, bq), 0)


def _attend(q_ref, k_ref, v_ref, o_ref, lse_ref, top_s, mix_s, *, kb, bq, scale):
    iq = pl.program_id(1)
    e = scale * LOG2E
    top_s[...] = jnp.full(top_s.shape, NEG, F32)
    mix_s[...] = jnp.zeros(mix_s.shape, F32)
    ones = jnp.ones((8, bq), BF)

    def block(j, masked):
        here = pl.ds(pl.multiple_of(j * bq, bq), bq)
        scores = [_dot(k_ref[here, _head(i)], q_ref[:, _head(i)], 1, 1) for i in range(kb)]
        ok = _below(bq, bq) if masked else None
        weights, keeps = [], []
        for i, s in enumerate(scores):
            if masked:
                s = jnp.where(ok, s, HIDDEN)
            old = top_s[i : i + 1, :]
            top = jnp.maximum(old, s.max(axis=0, keepdims=True))
            top_s[i : i + 1, :] = top
            weights.append(jnp.exp2((s - top) * e).astype(BF))
            keeps.append(jnp.exp2((old - top) * e))
        for i in range(kb):
            values = jnp.concatenate([v_ref[here, _head(i)].T, ones], axis=0)
            mix_s[i] = mix_s[i] * keeps[i] + _dot(values, weights[i])

    lax.fori_loop(0, iq, lambda j, _: block(j, False), None)
    block(iq, True)
    for i in range(kb):
        top, total = top_s[i : i + 1, :], mix_s[i, HEAD : HEAD + 1, :]
        o_ref[:, _head(i)] = (mix_s[i, :HEAD, :] * (1 / total)).T.astype(BF)
        lse_ref[0, i : i + 1, :] = top * scale + jnp.log(total)


def attend(q, k, v, kb=4, bq=512):
    tokens, cols = q.shape
    groups = cols // HEAD // kb
    some = pl.BlockSpec((bq, kb * HEAD), lambda h, n: (n, h))
    keys = pl.BlockSpec((tokens, kb * HEAD), lambda h, n: (0, h))
    return pl.pallas_call(
        functools.partial(_attend, kb=kb, bq=bq, scale=HEAD**-0.5),
        grid=(groups, tokens // bq),
        in_specs=[some, keys, keys],
        out_specs=[some, pl.BlockSpec((1, kb, bq), lambda h, n: (h, 0, n))],
        out_shape=[jax.ShapeDtypeStruct(q.shape, BF), jax.ShapeDtypeStruct((groups, kb, tokens), F32)],
        scratch_shapes=[pltpu.VMEM((kb, bq), F32), pltpu.VMEM((kb, HEAD + 8, bq), F32)],
        compiler_params=_params("arbitrary", "arbitrary"),
        cost_estimate=pl.CostEstimate(flops=8 * cols * tokens * tokens, transcendentals=groups * kb * tokens * tokens, bytes_accessed=8 * tokens * cols),
        name="attend",
    )(q, k, v)


def _attend_bwd(q_ref, k_ref, v_ref, o_ref, do_ref, lse_ref, cq_ref, sq_ref, cos_ref, sin_ref, dq_ref, dk_ref, dv_ref, dq_s, dk_s, dv_s, *, kb, bq, scale):
    iq = pl.program_id(1)
    e = scale * LOG2E

    @pl.when(iq == 0)
    def _():
        dk_s[...] = jnp.zeros_like(dk_s)
        dv_s[...] = jnp.zeros_like(dv_s)

    dq_s[...] = jnp.zeros_like(dq_s)
    lses = [lse_ref[0, i : i + 1, :] * LOG2E for i in range(kb)]
    deltas = [(do_ref[:, _head(i)].astype(F32) * o_ref[:, _head(i)].astype(F32)).T.sum(axis=0, keepdims=True) for i in range(kb)]

    def block(j, masked):
        here = pl.ds(pl.multiple_of(j * bq, bq), bq)
        scores = [_dot(k_ref[here, _head(i)], q_ref[:, _head(i)], 1, 1) for i in range(kb)]
        dps = [_dot(v_ref[here, _head(i)], do_ref[:, _head(i)], 1, 1) for i in range(kb)]
        ok = _below(bq, bq) if masked else None
        for i in range(kb):
            p = jnp.exp2(scores[i] * e - lses[i])
            if masked:
                p = jnp.where(ok, p, 0.0)
            ds = (p * (dps[i] - deltas[i])).astype(BF)
            dv_s[i, here, :] += _dot(p.astype(BF), do_ref[:, _head(i)])
            dk_s[i, here, :] += _dot(ds, q_ref[:, _head(i)])
            dq_s[i] += _dot(k_ref[here, _head(i)].T, ds)

    lax.fori_loop(0, iq, lambda j, _: block(j, False), None)
    block(iq, True)
    for i in range(kb):
        d = (dq_s[i] * scale).T
        dq_ref[:, _head(i)] = (d * cq_ref[...] + pltpu.roll(d * sq_ref[...], HEAD // 2, 1)).astype(BF)

    @pl.when(iq == pl.num_programs(1) - 1)
    def _():
        for i in range(kb):
            def some(n, _):
                here = pl.ds(pl.multiple_of(n * bq, bq), bq)
                d = dk_s[i, here, :] * scale
                dk_ref[here, _head(i)] = (d * cos_ref[here, :] + pltpu.roll(d * sin_ref[here, :], HEAD // 2, 1)).astype(BF)
                dv_ref[here, _head(i)] = dv_s[i, here, :].astype(BF)

            lax.fori_loop(0, dk_ref.shape[0] // bq, some, None)


def attend_bwd(q, k, v, o, lse, do, cos, sin, bq=512):
    tokens, cols = q.shape
    kb = lse.shape[1]
    groups = cols // HEAD // kb
    some = pl.BlockSpec((bq, kb * HEAD), lambda h, n: (n, h))
    keys = pl.BlockSpec((tokens, kb * HEAD), lambda h, n: (0, h))
    near = pl.BlockSpec((bq, HEAD), lambda h, n: (n, 0))
    whole = pl.BlockSpec((tokens, HEAD), lambda h, n: (0, 0))
    return pl.pallas_call(
        functools.partial(_attend_bwd, kb=kb, bq=bq, scale=HEAD**-0.5),
        grid=(groups, tokens // bq),
        in_specs=[some, keys, keys, some, some, pl.BlockSpec((1, kb, bq), lambda h, n: (h, 0, n)), near, near, whole, whole],
        out_specs=[some, keys, keys],
        out_shape=[jax.ShapeDtypeStruct(q.shape, BF)] * 3,
        scratch_shapes=[pltpu.VMEM((kb, HEAD, bq), F32), pltpu.VMEM((kb, tokens, HEAD), F32), pltpu.VMEM((kb, tokens, HEAD), F32)],
        compiler_params=_params("arbitrary", "arbitrary"),
        cost_estimate=pl.CostEstimate(flops=16 * cols * tokens * tokens, transcendentals=groups * kb * tokens * tokens, bytes_accessed=16 * tokens * cols),
        name="attend_bwd",
    )(q, k, v, o, do, lse, cos, sin, cos, sin)


def _mlp(place_ref, b_ref, dy_ref, go, uo, gr, ur, dn_ref, *rest, rows, given, begun):
    sums, rest = (rest[:4], rest[4:]) if given else (None, rest)
    db_in, rest = (rest[0], rest[1:]) if begun else (None, rest)
    db_ref, dg_ref, du_ref, dd_ref, dother_ref, gate_s, up_s, dg_s, du_s, dd_s, db_s = rest
    n, place = pl.program_id(0), place_ref[0]
    tokens, d = b_ref.shape
    half = d // 2
    mine, theirs = pl.ds(pl.multiple_of(place * half, half), half), pl.ds(pl.multiple_of((1 - place) * half, half), half)

    @pl.when(n == 0)
    def _():
        db_s[...] = db_in[...] if begun else jnp.zeros_like(db_s)

    dg_s[...] = jnp.zeros_like(dg_s)
    du_s[...] = jnp.zeros_like(du_s)
    dd_s[...] = sums[2][...] if given else jnp.zeros_like(dd_s)
    _whole(gate_s, go[...], gr[...], place)
    _whole(up_s, uo[...], ur[...], place)
    gate_t, up_t = gate_s[...].T, up_s[...].T

    def some(m, _):
        here = pl.ds(pl.multiple_of(m * rows, rows), rows)
        b, dy = b_ref[here, :], dy_ref[here, :]
        g = _dot(gate_t, b, 1, 1)
        u = _dot(up_t, b, 1, 1)
        dh = _dot(dn_ref[...], dy, 1, 1).astype(BF).astype(F32)
        s = jax.nn.sigmoid(g)
        silu = g * s
        hidden = (silu * u).astype(BF)
        du = (dh * silu).astype(BF)
        dg = (dh * u * (s + silu * (1 - s))).astype(BF)
        dd_s[...] += _dot(hidden, dy)
        dg_s[...] += _dot(dg, b)
        du_s[...] += _dot(du, b)
        db_s[:, here] += _dot(gate_s[...], dg) + _dot(up_s[...], du)

    lax.fori_loop(0, tokens // rows, some, None)
    for i, (s, out) in enumerate(((dg_s, dg_ref), (du_s, du_ref))):
        t = s[...].T
        s_own = jnp.where(place == 0, t[:half], t[half:])
        s_other = jnp.where(place == 0, t[half:], t[:half])
        out[...] = ((s_own + sums[i][...]) if given else s_own).astype(out.dtype)
        dother_ref[i] = ((s_other + sums[3][i]) if given else s_other).astype(dother_ref.dtype)
    dd_ref[...] = dd_s[...].astype(dd_ref.dtype)

    @pl.when(n == pl.num_programs(0) - 1)
    def _():
        db_ref[...] = db_s[...].T.astype(BF) if begun else db_s[...]


def mlp(place, b, dy, gate, up, other, down, part, sums=None, db=None, results=None, units=512, rows=512):
    tokens, d = b.shape
    hidden = down.shape[0] // 2
    steps = hidden // units
    final = sums is not None
    kind = BF if final else F32
    given = [*(sums or []), *([db] if db is not None else [])]
    kept = list(results) if results is not None else []
    whole = pl.BlockSpec((tokens, d), lambda n, p: (0, 0))
    whole_t = pl.BlockSpec((d, tokens), lambda n, p: (0, 0))
    own = pl.BlockSpec((d // 2, units), lambda n, p: (0, (2 * p[0] + part) * steps + n))
    got = [pl.BlockSpec((d // 2, units), functools.partial(lambda i, n, p: (0, i * steps + n), i)) for i in range(2)]
    w = pl.BlockSpec((d // 2, units), lambda n, p: (0, n))
    w2 = pl.BlockSpec((2, d // 2, units), lambda n, p: (0, 0, n))
    wd = pl.BlockSpec((units, d), lambda n, p: (n, 0))
    wd_in = pl.BlockSpec((units, d), lambda n, p: (part * steps + n, 0))
    shape = jax.ShapeDtypeStruct
    full = gate.shape if final else (d // 2, hidden)
    first = 8 + len(given)

    def kernel(*refs):
        _mlp(*refs[:first], *refs[first + len(kept) :], rows=rows, given=final, begun=db is not None)

    out, *dw = pl.pallas_call(
        kernel,
        grid_spec=pltpu.PrefetchScalarGridSpec(
            num_scalar_prefetch=1,
            grid=(steps,),
            in_specs=[whole, whole, own, own, *got, wd_in, *([w, w, wd, w2] if final else []), *([whole_t] if db is not None else []),
                      *[pl.BlockSpec(memory_space=pl.ANY)] * len(kept)],
            out_specs=[whole if db is not None else whole_t, *([own, own, wd_in] if final else [w, w, wd]), w2],
            scratch_shapes=[pltpu.VMEM((d, units), BF)] * 2 + [pltpu.VMEM((units, d), F32)] * 3 + [pltpu.VMEM((d, tokens), F32)],
        ),
        out_shape=[shape((tokens, d), BF) if db is not None else shape((d, tokens), F32), shape(full, kind), shape(full, kind),
                   shape((2 * hidden if final else hidden, d), kind), shape((2, d // 2, hidden), kind)],
        input_output_aliases={first + i: 1 + i for i in range(len(kept))},
        compiler_params=_params("arbitrary"),
        cost_estimate=pl.CostEstimate(flops=16 * tokens * d * hidden, transcendentals=tokens * hidden, bytes_accessed=30 * d * hidden),
        name="mlp",
    )(place, b, dy, gate, up, other, other, down, *given, *kept)
    return out, dw


def _proj_bwd(place_ref, a_ref, dq_ref, dk_ref, dv_ref, qo, ko, vo, other, *rest, given, begun):
    sums, rest = (rest[:4], rest[4:]) if given else (None, rest)
    da_in, rest = (rest[0], rest[1:]) if begun else (None, rest)
    da_ref, outs, dother_ref, w_s, accs = rest[0], rest[1:4], rest[4], rest[5], rest[6:]
    n, place = pl.program_id(0), place_ref[0]
    half = a_ref.shape[1] // 2
    cols = qo.shape[1]
    mine, theirs = pl.ds(pl.multiple_of(place * half, half), half), pl.ds(pl.multiple_of((1 - place) * half, half), half)
    part = [slice(i * cols, (i + 1) * cols) for i in range(3)]

    @pl.when(n == 0)
    def _():
        for i, (s, own) in enumerate(zip(accs, (qo, ko, vo))):
            _whole(w_s.at[:, part[i]], own[...], other[:, part[i]], place)
            if given:
                s[mine, :] = sums[i][...]
                s[theirs, :] = sums[3][:, part[i]]
            else:
                s[...] = jnp.zeros_like(s)

    a_t = a_ref[...].T
    ds = (dq_ref[...], dk_ref[...], dv_ref[...])
    da = sum(_dot(ds[i], w_s[:, part[i]], 1, 1) for i in range(3))
    da_ref[...] = (da + da_in[...]).astype(BF) if begun else da
    for i, s in enumerate(accs):
        s[...] += _dot(a_t, ds[i])

    @pl.when(n == pl.num_programs(0) - 1)
    def _():
        for i, s in enumerate(accs):
            outs[i][...] = s[mine, :].astype(outs[i].dtype)
            dother_ref[:, part[i]] = s[theirs, :].astype(dother_ref.dtype)


def proj_bwd(place, a, ds, own, other, part, sums=None, da=None, results=None, rows=512):
    tokens, d = a.shape
    cols = ds[0].shape[1]
    final = sums is not None
    kind = BF if final else F32
    given = [*(sums or []), *([da] if da is not None else [])]
    kept = list(results) if results is not None else []
    some = lambda wide: pl.BlockSpec((rows, wide), lambda n, p: (n, 0))
    mine = pl.BlockSpec((d // 2, cols), lambda n, p: (0, 2 * p[0] + part))
    w = pl.BlockSpec((d // 2, cols), lambda n, p: (0, 0))
    w3 = pl.BlockSpec((d // 2, 3 * cols), lambda n, p: (0, 0))
    shape = jax.ShapeDtypeStruct
    full = own[0].shape if final else (d // 2, cols)
    first = 9 + len(given)

    def kernel(*refs):
        _proj_bwd(*refs[:first], *refs[first + len(kept) :], given=final, begun=da is not None)

    out, *dw = pl.pallas_call(
        kernel,
        grid_spec=pltpu.PrefetchScalarGridSpec(
            num_scalar_prefetch=1,
            grid=(tokens // rows,),
            in_specs=[some(d), *[some(cols)] * 3, *[mine] * 3, w3, *([w, w, w, w3] if final else []), *([some(d)] if da is not None else []),
                      *[pl.BlockSpec(memory_space=pl.ANY)] * len(kept)],
            out_specs=[some(d), *[mine if final else w] * 3, w3],
            scratch_shapes=[pltpu.VMEM((d, 3 * cols), BF)] + [pltpu.VMEM((d, cols), F32)] * 3,
        ),
        out_shape=[shape((tokens, d), BF if da is not None else F32), *[shape(full, kind)] * 3, shape((d // 2, 3 * cols), kind)],
        input_output_aliases={first + i: 1 + i for i in range(len(kept))},
        compiler_params=_params("arbitrary"),
        cost_estimate=pl.CostEstimate(flops=12 * tokens * d * cols, transcendentals=0, bytes_accessed=2 * (2 * tokens * d + 9 * d * cols + 3 * tokens * cols)),
        name="proj_bwd",
    )(place, a, *ds, *own, other, *given, *kept)
    return out, dw


def normed(h):
    wide = h.astype(F32)
    scale = lax.rsqrt(jnp.mean(wide**2, -1, keepdims=True) + 1e-6)
    return (wide * scale).astype(BF)


def tables(tokens):
    half = HEAD // 2
    angle = jnp.arange(tokens, dtype=F32)[:, None] * THETA ** (-jnp.arange(half, dtype=F32) / half)
    cos, sin = jnp.cos(angle), jnp.sin(angle)
    return jnp.concatenate([cos, cos], 1), jnp.concatenate([-sin, sin], 1)


def after(t, *those):
    return lax.optimization_barrier((t, *those))[0]


def solution(mesh):
    swap = [(0, 1), (1, 0)]
    everyone = ("tp", "dp")

    def step(x, dy, wq, wk, wv, wo, wg, wu, wd):
        p = lax.axis_index("dp")
        place = p.astype(jnp.int32)[None]
        x, dy = x[0], dy[0]
        tokens = x.shape[0] * mesh.shape["tp"]

        def halves(t, axis, n):
            size = t.shape[axis] // 2
            return lax.dynamic_slice_in_dim(t, n * size, size, axis)

        def by_place(mine, theirs):
            return jnp.where(p == 0, mine, theirs), jnp.where(p == 0, theirs, mine)

        def runs(t, *those):
            return by_place(halves(t, 0, p), after(lax.ppermute(halves(t, 0, 1 - p), "dp", swap), *those))

        def gather(t):
            return lax.all_gather(t, everyone, axis=0, tiled=True)

        def collect(part):
            return lax.psum_scatter(part, everyone, scatter_dimension=0, tiled=True)

        def plus(t, more):
            return (t.astype(F32) + more.astype(F32)).astype(BF)

        def to_send(ws, part):
            size = ws[0].shape[1] // 4
            return jnp.concatenate([lax.dynamic_slice_in_dim(w, (2 * (1 - p) + part) * size, size, 1) for w in ws], 1)

        own, own2 = (wq, wk, wv), (wg, wu)
        send = [to_send(own, n) for n in (0, 1)]
        xs = runs(x, *send)
        other = []
        for n in (0, 1):
            other.append(lax.ppermute(send[n], "dp", swap))
        other2 = []
        for n in (0, 1):
            other2.append(lax.ppermute(to_send(own2, n), "dp", swap))
        norms, backs = zip(*(jax.vjp(normed, t) for t in xs))
        a = [gather(t) for t in norms]
        cos, sin = tables(tokens)
        wos = [wo[: wo.shape[0] // 2], wo[wo.shape[0] // 2 :]]

        def project(o):
            return (_dot(o[0][0], wos[0]) + _dot(o[1][0], wos[1])).astype(BF)

        def heads(a, n):
            t = qkv(place, a, own, other[n], cos, sin, n)
            return t, attend(*t)

        t00, o00 = heads(a[0], 0)
        dys = runs(dy, o00[0])
        t01, o01 = heads(after(a[0], *dys), 1)
        dy_all = [gather(dys[0])]
        h0 = collect(project((o00, o01)))
        dy_all.append(gather(after(dys[1], h0)))
        t10, o10 = heads(after(a[1], o01[0]), 0)
        t11 = qkv(place, after(a[1], o10[0]), own, other[1], cos, sin, 1)
        h0 = plus(xs[0], after(h0, t11[0]))
        b0, back0 = jax.vjp(normed, h0)
        o11 = attend(after(t11[0], b0), *t11[1:])
        b0 = gather(b0)
        h1 = collect(project((o10, o11)))
        db0, w0a = mlp(place, b0, dy_all[0], wg, wu, other2[0], wd, 0)
        h1 = plus(xs[1], after(h1, db0))
        b1, back1 = jax.vjp(normed, h1)
        db0, w0b = mlp(place, after(b0, b1), dy_all[0], wg, wu, other2[1], wd, 1, None, db0)
        b1 = gather(b1)
        db0 = collect(db0)
        db1, w1a = mlp(place, b1, dy_all[1], wg, wu, other2[0], wd, 0, w0a)
        ga = lax.ppermute(w1a[3], "dp", swap)
        dh0 = plus(dys[0], back0(after(db0, db1))[0])
        db1, w1b = mlp(place, after(b1, dh0), dy_all[1], wg, wu, other2[1], wd, 1, w0b, db1, w1a[:3])
        d0 = gather(dh0)
        gb = lax.ppermute(w1b[3], "dp", swap)
        db1 = collect(db1)

        def heads_back(t, o, d, n):
            do = _dot(d, wos[n], 1, 1).astype(BF)
            return attend_bwd(*t, *o, do, cos, sin)

        ds0 = heads_back(t00, o00, d0, 0)
        dh1 = plus(dys[1], back1(after(db1, ds0[0]))[0])
        ds1 = heads_back((after(t01[0], dh1), *t01[1:]), o01, d0, 1)
        d1 = gather(dh1)
        da0, s0 = proj_bwd(place, a[0], ds0, own, other[0], 0)
        da0, s1 = proj_bwd(place, a[0], ds1, own, other[1], 1, None, da0)
        da0 = collect(da0)
        ds0 = heads_back(t10, o10, d1, 0)
        da1, s0 = proj_bwd(place, a[1], ds0, own, other[0], 0, s0)
        g0 = lax.ppermute(s0[3], "dp", swap)
        ds1 = heads_back((after(t11[0], da1), *t11[1:]), o11, d1, 1)
        da1, s1 = proj_bwd(place, a[1], ds1, own, other[1], 1, s1, da1, s0[:3])
        da1 = collect(da1)
        g1 = lax.ppermute(s1[3], "dp", swap)
        dx0 = plus(dh0, backs[0](da0)[0])
        dx1 = plus(dh1, backs[1](da1)[0])
        mine, theirs = by_place(dx0, dx1)
        theirs = lax.ppermute(theirs, "dp", swap)
        dx = jnp.concatenate(by_place(mine, theirs), 0)
        dwo = jnp.concatenate([(_dot(m[0], d0, 0, 0) + _dot(n[0], d1, 0, 0)).astype(BF) for m, n in ((o00, o10), (o01, o11))], 0)

        def with_other(full, *got):
            size = got[0].shape[1]
            for n, t in enumerate(got):
                full = lax.dynamic_update_slice(full, t, (0, (2 * (1 - p) + n) * size))
            return full

        cols = g0.shape[1] // 3
        dw = [with_other(s1[i], *(g[:, i * cols : (i + 1) * cols] for g in (g0, g1))) for i in range(3)]
        ga, gb = after(ga, da1), after(gb, da1)
        dwg, dwu = (with_other(w1b[i], ga[i], gb[i]) for i in range(2))
        return (dx[None], *dw, dwo, dwg, dwu, w1b[2])

    states, by_columns, by_rows = P("dp", "tp", None), P("dp", "tp"), P(("tp", "dp"), None)
    weights = (by_columns, by_columns, by_columns, by_rows, by_columns, by_columns, by_rows)
    return jax.shard_map(step, mesh=mesh, in_specs=(states, states, *weights), out_specs=(states, *weights), check_vma=False)
```

```python
import functools

import jax
import jax.numpy as jnp
from jax import lax
from jax.experimental import pallas as pl
from jax.experimental.pallas import tpu as pltpu
from jax.sharding import PartitionSpec as P

HEAD = 128
THETA = 10000
NEG = -1e30
HIDDEN = 2 * NEG
LOG2E = 1.4426950408889634
VMEM = 60 * 2**20
STEP = 256
BF, F32 = jnp.bfloat16, jnp.float32


def _dot(a, b, ca=1, cb=0):
    return lax.dot_general(a, b, (((ca,), (cb,)), ((), ())), preferred_element_type=F32)


def _params(*kinds):
    return pltpu.CompilerParams(dimension_semantics=kinds, vmem_limit_bytes=VMEM)


def _head(i):
    return slice(i * HEAD, (i + 1) * HEAD)


def _whole(scratch, own, other, place):
    half = own.shape[0]
    scratch[pl.ds(pl.multiple_of(place * half, half), half), :] = own
    scratch[pl.ds(pl.multiple_of((1 - place) * half, half), half), :] = other


def _below(bk, bq):
    return lax.broadcasted_iota(jnp.int32, (bk, bq), 1) >= lax.broadcasted_iota(jnp.int32, (bk, bq), 0)


def _heads(place_ref, a_ref, qo, ko, vo, other, cos_ref, sin_ref, q_ref, k_ref, v_ref, o_ref, lse_ref, w_s, k_s, v_s, top_s, mix_s, *, kb, bq, rows, scale):
    iq = pl.program_id(0)
    cols = kb * HEAD

    @pl.when(iq == 0)
    def _():
        for i, own in enumerate((qo, ko, vo)):
            part = slice(i * cols, (i + 1) * cols)
            _whole(w_s.at[:, part], own[...], other[:, part], place_ref[0])

    def some(n, _):
        here = pl.ds(pl.multiple_of(n * rows, rows), rows)
        there = pl.ds(pl.multiple_of(iq * bq + n * rows, rows), rows)
        cos, sin = cos_ref[here, :], sin_ref[here, :]
        for i, out in enumerate((q_ref, k_ref, v_ref)):
            t = _dot(a_ref[here, :], w_s[:, i * cols : (i + 1) * cols]).astype(BF)
            for h in range(kb):
                u = t[:, _head(h)]
                if i < 2:
                    u = u.astype(F32)
                    u = (u * cos + pltpu.roll(u, HEAD // 2, 1) * sin).astype(BF)
                out[here, _head(h)] = u
                if i > 0:
                    (k_s if i == 1 else v_s)[there, _head(h)] = u

    lax.fori_loop(0, bq // rows, some, None)
    e = scale * LOG2E
    top_s[...] = jnp.full(top_s.shape, NEG, F32)
    mix_s[...] = jnp.zeros(mix_s.shape, F32)

    def block(start, size, lo, masked):
        here = pl.ds(pl.multiple_of(start, size), size)
        scores = [_dot(k_s[here, _head(i)], q_ref[lo:, _head(i)], 1, 1) for i in range(kb)]
        ok = _below(size, bq - lo) if masked else None
        ones = jnp.ones((8, size), BF)
        weights, keeps = [], []
        for i, s in enumerate(scores):
            if masked:
                s = jnp.where(ok, s, HIDDEN)
            old = top_s[i : i + 1, lo:]
            top = jnp.maximum(old, s.max(axis=0, keepdims=True))
            top_s[i : i + 1, lo:] = top
            weights.append(jnp.exp2((s - top) * e).astype(BF))
            keeps.append(jnp.exp2((old - top) * e))
        for i in range(kb):
            values = jnp.concatenate([v_s[here, _head(i)].T, ones], axis=0)
            mix_s[i, :, lo:] = mix_s[i, :, lo:] * keeps[i] + _dot(values, weights[i])

    lax.fori_loop(0, iq, lambda j, _: block(j * bq, bq, 0, False), None)
    for lo in range(0, bq, STEP):
        block(iq * bq + lo, STEP, lo, True)
    for i in range(kb):
        top, total = top_s[i : i + 1, :], mix_s[i, HEAD : HEAD + 1, :]
        o_ref[:, _head(i)] = (mix_s[i, :HEAD, :] * (1 / total)).T.astype(BF)
        lse_ref[i : i + 1, :] = top * scale + jnp.log(total)


def heads(place, a, own, other, cos, sin, part, bq=1024, rows=512):
    tokens, d = a.shape
    cols = other.shape[1] // 3
    kb = cols // HEAD
    some = lambda wide: pl.BlockSpec((bq, wide), lambda n, p: (n, 0))
    mine = pl.BlockSpec((d // 2, cols), lambda n, p: (0, 2 * p[0] + part))
    q, k, v, o, lse = pl.pallas_call(
        functools.partial(_heads, kb=kb, bq=bq, rows=rows, scale=HEAD**-0.5),
        grid_spec=pltpu.PrefetchScalarGridSpec(
            num_scalar_prefetch=1,
            grid=(tokens // bq,),
            in_specs=[some(d), *[mine] * 3, pl.BlockSpec(other.shape, lambda n, p: (0, 0)), some(HEAD), some(HEAD)],
            out_specs=[*[some(cols)] * 4, pl.BlockSpec((kb, bq), lambda n, p: (0, n))],
            scratch_shapes=[pltpu.VMEM((d, 3 * cols), BF), pltpu.VMEM((tokens, cols), BF), pltpu.VMEM((tokens, cols), BF), pltpu.VMEM((kb, bq), F32),
                            pltpu.VMEM((kb, HEAD + 8, bq), F32)],
        ),
        out_shape=[*[jax.ShapeDtypeStruct((tokens, cols), BF)] * 4, jax.ShapeDtypeStruct((kb, tokens), F32)],
        compiler_params=_params("arbitrary"),
        cost_estimate=pl.CostEstimate(flops=6 * tokens * d * cols + 8 * cols * tokens * tokens, transcendentals=kb * tokens * tokens,
                                      bytes_accessed=2 * (tokens * d + 3 * d * cols + 4 * tokens * cols)),
        name="heads",
    )(place, a, *own, other, cos, sin)
    return (q, k, v), (o, lse)


def _attend_bwd(q_ref, k_ref, v_ref, o_ref, lse_ref, d_ref, wo_ref, cq_ref, sq_ref, cos_ref, sin_ref, dq_ref, dk_ref, dv_ref, do_ref, dq_s, dk_s, dv_s, *, kb, bq, scale):
    iq = pl.program_id(0)
    e = scale * LOG2E

    @pl.when(iq == 0)
    def _():
        dk_s[...] = jnp.zeros_like(dk_s)
        dv_s[...] = jnp.zeros_like(dv_s)

    dq_s[...] = jnp.zeros_like(dq_s)
    do_ref[...] = _dot(d_ref[...], wo_ref[...], 1, 1).astype(BF)
    lses = [lse_ref[i : i + 1, :] * LOG2E for i in range(kb)]
    deltas = [(do_ref[:, _head(i)].astype(F32) * o_ref[:, _head(i)].astype(F32)).T.sum(axis=0, keepdims=True) for i in range(kb)]

    def block(start, size, lo, masked):
        here = pl.ds(pl.multiple_of(start, size), size)
        scores = [_dot(k_ref[here, _head(i)], q_ref[lo:, _head(i)], 1, 1) for i in range(kb)]
        dps = [_dot(v_ref[here, _head(i)], do_ref[lo:, _head(i)], 1, 1) for i in range(kb)]
        ok = _below(size, bq - lo) if masked else None
        for i in range(kb):
            p = jnp.exp2(scores[i] * e - lses[i][:, lo:])
            if masked:
                p = jnp.where(ok, p, 0.0)
            ds = (p * (dps[i] - deltas[i][:, lo:])).astype(BF)
            dv_s[i, here, :] += _dot(p.astype(BF), do_ref[lo:, _head(i)])
            dk_s[i, here, :] += _dot(ds, q_ref[lo:, _head(i)])
            dq_s[i, :, lo:] += _dot(k_ref[here, _head(i)].T, ds)

    lax.fori_loop(0, iq, lambda j, _: block(j * bq, bq, 0, False), None)
    for lo in range(0, bq, STEP):
        block(iq * bq + lo, STEP, lo, True)
    for i in range(kb):
        d = (dq_s[i] * scale).T
        dq_ref[:, _head(i)] = (d * cq_ref[...] + pltpu.roll(d * sq_ref[...], HEAD // 2, 1)).astype(BF)

    @pl.when(iq == pl.num_programs(0) - 1)
    def _():
        for i in range(kb):
            def some(n, _):
                here = pl.ds(pl.multiple_of(n * bq, bq), bq)
                d = dk_s[i, here, :] * scale
                dk_ref[here, _head(i)] = (d * cos_ref[here, :] + pltpu.roll(d * sin_ref[here, :], HEAD // 2, 1)).astype(BF)
                dv_ref[here, _head(i)] = dv_s[i, here, :].astype(BF)

            lax.fori_loop(0, dk_ref.shape[0] // bq, some, None)


def attend_bwd(q, k, v, o, lse, d, wo, cos, sin, part, bq=512):
    tokens, cols = q.shape
    kb = lse.shape[0]
    width = d.shape[1]
    some = pl.BlockSpec((bq, cols), lambda n: (n, 0))
    keys = pl.BlockSpec((tokens, cols), lambda n: (0, 0))
    near = pl.BlockSpec((bq, HEAD), lambda n: (n, 0))
    whole = pl.BlockSpec((tokens, HEAD), lambda n: (0, 0))
    return pl.pallas_call(
        functools.partial(_attend_bwd, kb=kb, bq=bq, scale=HEAD**-0.5),
        grid=(tokens // bq,),
        in_specs=[some, keys, keys, some, pl.BlockSpec((kb, bq), lambda n: (0, n)), pl.BlockSpec((bq, width), lambda n: (n, 0)),
                  pl.BlockSpec((cols, width), lambda n: (part, 0)), near, near, whole, whole],
        out_specs=[some, keys, keys],
        out_shape=[jax.ShapeDtypeStruct(q.shape, BF)] * 3,
        scratch_shapes=[pltpu.VMEM((bq, cols), BF), pltpu.VMEM((kb, HEAD, bq), F32), pltpu.VMEM((kb, tokens, HEAD), F32), pltpu.VMEM((kb, tokens, HEAD), F32)],
        compiler_params=_params("arbitrary"),
        cost_estimate=pl.CostEstimate(flops=16 * cols * tokens * tokens, transcendentals=kb * tokens * tokens, bytes_accessed=16 * tokens * cols),
        name="attend_bwd",
    )(q, k, v, o, lse, d, wo, cos, sin, cos, sin)


def _mlp(place_ref, b_ref, dy_ref, go, uo, gr, ur, dn_ref, *rest, rows, given, begun):
    sums, rest = (rest[:4], rest[4:]) if given else (None, rest)
    db_in, rest = (rest[0], rest[1:]) if begun else (None, rest)
    db_ref, dg_ref, du_ref, dd_ref, dother_ref, gate_s, up_s, dg_s, du_s, dd_s, db_s = rest
    n, place = pl.program_id(0), place_ref[0]
    tokens, d = b_ref.shape
    half = d // 2
    mine, theirs = pl.ds(pl.multiple_of(place * half, half), half), pl.ds(pl.multiple_of((1 - place) * half, half), half)

    @pl.when(n == 0)
    def _():
        db_s[...] = db_in[...] if begun else jnp.zeros_like(db_s)

    dg_s[...] = jnp.zeros_like(dg_s)
    du_s[...] = jnp.zeros_like(du_s)
    dd_s[...] = sums[2][...] if given else jnp.zeros_like(dd_s)
    _whole(gate_s, go[...], gr[...], place)
    _whole(up_s, uo[...], ur[...], place)
    gate_t, up_t = gate_s[...].T, up_s[...].T

    def first(m):
        here = pl.ds(m * rows, rows)
        b, dy = b_ref[here, :], dy_ref[here, :]
        g = _dot(gate_t, b, 1, 1)
        u = _dot(up_t, b, 1, 1)
        dh = _dot(dn_ref[...], dy, 1, 1).astype(BF).astype(F32)
        s = 0.5 * jnp.tanh(0.5 * g) + 0.5
        silu = g * s
        return (silu * u).astype(BF), (dh * u * (s + silu * (1 - s))).astype(BF), (dh * silu).astype(BF)

    def second(m, hidden, dg, du):
        here = pl.ds(m * rows, rows)
        b, dy = b_ref[here, :], dy_ref[here, :]
        dd_s[...] += _dot(hidden, dy)
        dg_s[...] += _dot(dg, b)
        du_s[...] += _dot(du, b)
        db_s[:, here] += _dot(gate_s[...], dg) + _dot(up_s[...], du)

    now = first(0)
    for m in range(tokens // rows):
        then = first(m + 1) if m + 1 < tokens // rows else None
        second(m, *now)
        now = then

    for i, (s, out) in enumerate(((dg_s, dg_ref), (du_s, du_ref))):
        t = s[...].T
        s_own = jnp.where(place == 0, t[:half], t[half:])
        s_other = jnp.where(place == 0, t[half:], t[:half])
        out[...] = ((s_own + sums[i][...]) if given else s_own).astype(out.dtype)
        dother_ref[i] = ((s_other + sums[3][i]) if given else s_other).astype(dother_ref.dtype)
    dd_ref[...] = dd_s[...].astype(dd_ref.dtype)

    @pl.when(n == pl.num_programs(0) - 1)
    def _():
        db_ref[...] = db_s[...].T.astype(BF) if begun else db_s[...]


def mlp(place, b, dy, gate, up, other, down, part, sums=None, db=None, results=None, units=512, rows=512):
    tokens, d = b.shape
    hidden = down.shape[0] // 2
    steps = hidden // units
    final = sums is not None
    kind = BF if final else F32
    given = [*(sums or []), *([db] if db is not None else [])]
    kept = list(results) if results is not None else []
    whole = pl.BlockSpec((tokens, d), lambda n, p: (0, 0))
    whole_t = pl.BlockSpec((d, tokens), lambda n, p: (0, 0))
    own = pl.BlockSpec((d // 2, units), lambda n, p: (0, (2 * p[0] + part) * steps + n))
    got = [pl.BlockSpec((d // 2, units), functools.partial(lambda i, n, p: (0, i * steps + n), i)) for i in range(2)]
    w = pl.BlockSpec((d // 2, units), lambda n, p: (0, n))
    w2 = pl.BlockSpec((2, d // 2, units), lambda n, p: (0, 0, n))
    wd = pl.BlockSpec((units, d), lambda n, p: (n, 0))
    wd_in = pl.BlockSpec((units, d), lambda n, p: (part * steps + n, 0))
    shape = jax.ShapeDtypeStruct
    full = gate.shape if final else (d // 2, hidden)
    first = 8 + len(given)

    def kernel(*refs):
        _mlp(*refs[:first], *refs[first + len(kept) :], rows=rows, given=final, begun=db is not None)

    out, *dw = pl.pallas_call(
        kernel,
        grid_spec=pltpu.PrefetchScalarGridSpec(
            num_scalar_prefetch=1,
            grid=(steps,),
            in_specs=[whole, whole, own, own, *got, wd_in, *([w, w, wd, w2] if final else []), *([whole_t] if db is not None else []),
                      *[pl.BlockSpec(memory_space=pl.ANY)] * len(kept)],
            out_specs=[whole if db is not None else whole_t, *([own, own, wd_in] if final else [w, w, wd]), w2],
            scratch_shapes=[pltpu.VMEM((d, units), BF)] * 2 + [pltpu.VMEM((units, d), F32)] * 3 + [pltpu.VMEM((d, tokens), F32)],
        ),
        out_shape=[shape((tokens, d), BF) if db is not None else shape((d, tokens), F32), shape(full, kind), shape(full, kind),
                   shape((2 * hidden if final else hidden, d), kind), shape((2, d // 2, hidden), kind)],
        input_output_aliases={first + i: 1 + i for i in range(len(kept))},
        compiler_params=_params("arbitrary"),
        cost_estimate=pl.CostEstimate(flops=16 * tokens * d * hidden, transcendentals=tokens * hidden, bytes_accessed=30 * d * hidden),
        name="mlp",
    )(place, b, dy, gate, up, other, other, down, *given, *kept)
    return out, dw


def _proj_bwd(place_ref, a_ref, dq_ref, dk_ref, dv_ref, qo, ko, vo, other, *rest, given, begun):
    sums, rest = (rest[:4], rest[4:]) if given else (None, rest)
    da_in, rest = (rest[0], rest[1:]) if begun else (None, rest)
    da_ref, outs, dother_ref, w_s, accs = rest[0], rest[1:4], rest[4], rest[5], rest[6:]
    n, place = pl.program_id(0), place_ref[0]
    half = a_ref.shape[1] // 2
    cols = qo.shape[1]
    mine, theirs = pl.ds(pl.multiple_of(place * half, half), half), pl.ds(pl.multiple_of((1 - place) * half, half), half)
    part = [slice(i * cols, (i + 1) * cols) for i in range(3)]

    @pl.when(n == 0)
    def _():
        for i, (s, own) in enumerate(zip(accs, (qo, ko, vo))):
            _whole(w_s.at[:, part[i]], own[...], other[:, part[i]], place)
            if given:
                s[mine, :] = sums[i][...]
                s[theirs, :] = sums[3][:, part[i]]
            else:
                s[...] = jnp.zeros_like(s)

    a_t = a_ref[...].T
    ds = (dq_ref[...], dk_ref[...], dv_ref[...])
    da = sum(_dot(ds[i], w_s[:, part[i]], 1, 1) for i in range(3))
    da_ref[...] = (da + da_in[...]).astype(BF) if begun else da
    for i, s in enumerate(accs):
        s[...] += _dot(a_t, ds[i])

    @pl.when(n == pl.num_programs(0) - 1)
    def _():
        for i, s in enumerate(accs):
            outs[i][...] = s[mine, :].astype(outs[i].dtype)
            dother_ref[:, part[i]] = s[theirs, :].astype(dother_ref.dtype)


def proj_bwd(place, a, ds, own, other, part, sums=None, da=None, results=None, rows=512):
    tokens, d = a.shape
    cols = ds[0].shape[1]
    final = sums is not None
    kind = BF if final else F32
    given = [*(sums or []), *([da] if da is not None else [])]
    kept = list(results) if results is not None else []
    some = lambda wide: pl.BlockSpec((rows, wide), lambda n, p: (n, 0))
    mine = pl.BlockSpec((d // 2, cols), lambda n, p: (0, 2 * p[0] + part))
    w = pl.BlockSpec((d // 2, cols), lambda n, p: (0, 0))
    w3 = pl.BlockSpec((d // 2, 3 * cols), lambda n, p: (0, 0))
    shape = jax.ShapeDtypeStruct
    full = own[0].shape if final else (d // 2, cols)
    first = 9 + len(given)

    def kernel(*refs):
        _proj_bwd(*refs[:first], *refs[first + len(kept) :], given=final, begun=da is not None)

    out, *dw = pl.pallas_call(
        kernel,
        grid_spec=pltpu.PrefetchScalarGridSpec(
            num_scalar_prefetch=1,
            grid=(tokens // rows,),
            in_specs=[some(d), *[some(cols)] * 3, *[mine] * 3, w3, *([w, w, w, w3] if final else []), *([some(d)] if da is not None else []),
                      *[pl.BlockSpec(memory_space=pl.ANY)] * len(kept)],
            out_specs=[some(d), *[mine if final else w] * 3, w3],
            scratch_shapes=[pltpu.VMEM((d, 3 * cols), BF)] + [pltpu.VMEM((d, cols), F32)] * 3,
        ),
        out_shape=[shape((tokens, d), BF if da is not None else F32), *[shape(full, kind)] * 3, shape((d // 2, 3 * cols), kind)],
        input_output_aliases={first + i: 1 + i for i in range(len(kept))},
        compiler_params=_params("arbitrary"),
        cost_estimate=pl.CostEstimate(flops=12 * tokens * d * cols, transcendentals=0, bytes_accessed=2 * (2 * tokens * d + 9 * d * cols + 3 * tokens * cols)),
        name="proj_bwd",
    )(place, a, *ds, *own, other, *given, *kept)
    return out, dw


def normed(h):
    wide = h.astype(F32)
    scale = lax.rsqrt(jnp.mean(wide**2, -1, keepdims=True) + 1e-6)
    return (wide * scale).astype(BF)


def tables(tokens):
    half = HEAD // 2
    angle = jnp.arange(tokens, dtype=F32)[:, None] * THETA ** (-jnp.arange(half, dtype=F32) / half)
    cos, sin = jnp.cos(angle), jnp.sin(angle)
    return jnp.concatenate([cos, cos], 1), jnp.concatenate([-sin, sin], 1)


def after(t, *those):
    return lax.optimization_barrier((t, *those))[0]


def solution(mesh):
    swap = [(0, 1), (1, 0)]
    everyone = ("tp", "dp")

    def step(x, dy, wq, wk, wv, wo, wg, wu, wd):
        p = lax.axis_index("dp")
        place = p.astype(jnp.int32)[None]
        x, dy = x[0], dy[0]
        tokens = x.shape[0] * mesh.shape["tp"]

        def halves(t, axis, n):
            size = t.shape[axis] // 2
            return lax.dynamic_slice_in_dim(t, n * size, size, axis)

        def by_place(mine, theirs):
            return jnp.where(p == 0, mine, theirs), jnp.where(p == 0, theirs, mine)

        def runs(t, *those):
            return by_place(halves(t, 0, p), after(lax.ppermute(halves(t, 0, 1 - p), "dp", swap), *those))

        def gather(t):
            return lax.all_gather(t, everyone, axis=0, tiled=True)

        def collect(part):
            return lax.psum_scatter(part, everyone, scatter_dimension=0, tiled=True)

        def plus(t, more):
            return (t.astype(F32) + more.astype(F32)).astype(BF)

        def to_send(ws, part):
            size = ws[0].shape[1] // 4
            return jnp.concatenate([lax.dynamic_slice_in_dim(w, (2 * (1 - p) + part) * size, size, 1) for w in ws], 1)

        own, own2 = (wq, wk, wv), (wg, wu)
        send = [to_send(own, n) for n in (0, 1)]
        xs = runs(x, *send)
        other = []
        for n in (0, 1):
            other.append(lax.ppermute(send[n], "dp", swap))
        other2 = []
        for n in (0, 1):
            other2.append(lax.ppermute(to_send(own2, n), "dp", swap))
        norms, backs = zip(*(jax.vjp(normed, t) for t in xs))
        a = [gather(t) for t in norms]
        cos, sin = tables(tokens)
        half = wo.shape[0] // 2

        def project(o):
            return (_dot(o[0][0], wo[:half]) + _dot(o[1][0], wo[half:])).astype(BF)

        def half_heads(a, n):
            return heads(place, a, own, other[n], cos, sin, n)

        t00, o00 = half_heads(after(a[0], norms[1]), 0)
        dys = runs(dy, o00[0])
        t01, o01 = half_heads(after(a[0], *dys), 1)
        dy_all = [gather(dys[0])]
        h0 = collect(after(project((o00, o01)), dy_all[0]))
        dy_all.append(gather(after(dys[1], h0)))
        t10, o10 = half_heads(after(a[1], o01[0]), 0)
        h0 = plus(xs[0], after(h0, o10[0]))
        b0, back0 = jax.vjp(normed, h0)
        t11, o11 = half_heads(after(a[1], b0), 1)
        b0 = gather(b0)
        h1 = collect(project((o10, o11)))
        db0, w0a = mlp(place, b0, dy_all[0], wg, wu, other2[0], wd, 0)
        h1 = plus(xs[1], after(h1, db0))
        b1, back1 = jax.vjp(normed, h1)
        db0, w0b = mlp(place, after(b0, b1), dy_all[0], wg, wu, other2[1], wd, 1, None, db0)
        b1 = gather(b1)
        db0 = collect(db0)
        db1, w1a = mlp(place, b1, dy_all[1], wg, wu, other2[0], wd, 0, w0a)
        ga = lax.ppermute(w1a[3], "dp", swap)
        dh0 = plus(dys[0], back0(after(db0, db1))[0])
        db1, w1b = mlp(place, after(b1, dh0), dy_all[1], wg, wu, other2[1], wd, 1, w0b, db1, w1a[:3])
        d0 = gather(dh0)
        gb = lax.ppermute(w1b[3], "dp", swap)
        db1 = collect(db1)

        def heads_back(t, o, d, n):
            return attend_bwd(*t, *o, d, wo, cos, sin, n)

        ds0 = heads_back(t00, o00, d0, 0)
        dh1 = plus(dys[1], back1(after(db1, ds0[0]))[0])
        ds1 = heads_back((after(t01[0], dh1), *t01[1:]), o01, d0, 1)
        d1 = gather(dh1)
        da0, s0 = proj_bwd(place, a[0], ds0, own, other[0], 0)
        da0, s1 = proj_bwd(place, a[0], ds1, own, other[1], 1, None, da0)
        da0 = collect(da0)
        ds0 = heads_back(t10, o10, d1, 0)
        da1, s0 = proj_bwd(place, a[1], ds0, own, other[0], 0, s0)
        g0 = lax.ppermute(s0[3], "dp", swap)
        ds1 = heads_back((after(t11[0], da1), *t11[1:]), o11, d1, 1)
        da1, s1 = proj_bwd(place, a[1], ds1, own, other[1], 1, s1, da1, s0[:3])
        da1 = collect(da1)
        g1 = lax.ppermute(s1[3], "dp", swap)
        dx0 = plus(dh0, backs[0](da0)[0])
        dx1 = plus(dh1, backs[1](da1)[0])
        mine, theirs = by_place(dx0, dx1)
        theirs = lax.ppermute(theirs, "dp", swap)
        dx = jnp.concatenate(by_place(mine, theirs), 0)
        dwo = jnp.concatenate([(_dot(m[0], d0, 0, 0) + _dot(n[0], d1, 0, 0)).astype(BF) for m, n in ((o00, o10), (o01, o11))], 0)

        def with_other(full, *got):
            size = got[0].shape[1]
            for n, t in enumerate(got):
                full = lax.dynamic_update_slice(full, t, (0, (2 * (1 - p) + n) * size))
            return full

        cols = g0.shape[1] // 3
        dw = [with_other(s1[i], *(g[:, i * cols : (i + 1) * cols] for g in (g0, g1))) for i in range(3)]
        ga, gb = after(ga, da1), after(gb, da1)
        dwg, dwu = (with_other(w1b[i], ga[i], gb[i]) for i in range(2))
        return (dx[None], *dw, dwo, dwg, dwu, w1b[2])

    states, by_columns, by_rows = P("dp", "tp", None), P("dp", "tp"), P(("tp", "dp"), None)
    weights = (by_columns, by_columns, by_columns, by_rows, by_columns, by_columns, by_rows)
    return jax.shard_map(step, mesh=mesh, in_specs=(states, states, *weights), out_specs=(states, *weights), check_vma=False)
```

```python
import functools

import jax
import jax.numpy as jnp
from jax import lax
from jax.experimental import pallas as pl
from jax.experimental.pallas import tpu as pltpu
from jax.sharding import PartitionSpec as P

HEAD = 128
THETA = 10000
NEG = -1e30
HIDDEN = 2 * NEG
LOG2E = 1.4426950408889634
VMEM = 60 * 2**20
STEP = 256
BF, F32 = jnp.bfloat16, jnp.float32


def _dot(a, b, ca=1, cb=0):
    return lax.dot_general(a, b, (((ca,), (cb,)), ((), ())), preferred_element_type=F32)


def _params(*kinds):
    return pltpu.CompilerParams(dimension_semantics=kinds, vmem_limit_bytes=VMEM)


def _head(i):
    return slice(i * HEAD, (i + 1) * HEAD)


def _whole(scratch, own, other, place):
    half = own.shape[0]
    scratch[pl.ds(pl.multiple_of(place * half, half), half), :] = own
    scratch[pl.ds(pl.multiple_of((1 - place) * half, half), half), :] = other


def _below(bk, bq):
    return lax.broadcasted_iota(jnp.int32, (bk, bq), 1) >= lax.broadcasted_iota(jnp.int32, (bk, bq), 0)


def _heads(place_ref, a_ref, qo, ko, vo, other, cos_ref, sin_ref, *rest, kb, bq, rows, scale, joined):
    before, wo_ref = rest[:2] if joined else (None, None)
    q_ref, k_ref, v_ref, o_ref, lse_ref = rest[2:7] if joined else rest[:5]
    w_s, k_s, v_s, top_s, mix_s = rest[-5:]
    iq = pl.program_id(0)
    cols = kb * HEAD

    @pl.when(iq == 0)
    def _():
        for i, own in enumerate((qo, ko, vo)):
            part = slice(i * cols, (i + 1) * cols)
            _whole(w_s.at[:, part], own[...], other[:, part], place_ref[0])

    def some(n, _):
        here = pl.ds(pl.multiple_of(n * rows, rows), rows)
        there = pl.ds(pl.multiple_of(iq * bq + n * rows, rows), rows)
        cos, sin = cos_ref[here, :], sin_ref[here, :]
        for i, out in enumerate((q_ref, k_ref, v_ref)):
            t = _dot(a_ref[here, :], w_s[:, i * cols : (i + 1) * cols]).astype(BF)
            for h in range(kb):
                u = t[:, _head(h)]
                if i < 2:
                    u = u.astype(F32)
                    u = (u * cos + pltpu.roll(u, HEAD // 2, 1) * sin).astype(BF)
                out[here, _head(h)] = u
                if i > 0:
                    (k_s if i == 1 else v_s)[there, _head(h)] = u

    lax.fori_loop(0, bq // rows, some, None)
    e = scale * LOG2E
    top_s[...] = jnp.full(top_s.shape, NEG, F32)
    mix_s[...] = jnp.zeros(mix_s.shape, F32)

    def block(start, size, lo, masked):
        here = pl.ds(pl.multiple_of(start, size), size)
        scores = [_dot(k_s[here, _head(i)], q_ref[lo:, _head(i)], 1, 1) for i in range(kb)]
        ok = _below(size, bq - lo) if masked else None
        ones = jnp.ones((8, size), BF)
        weights, keeps = [], []
        for i, s in enumerate(scores):
            if masked:
                s = jnp.where(ok, s, HIDDEN)
            old = top_s[i : i + 1, lo:]
            top = jnp.maximum(old, s.max(axis=0, keepdims=True))
            top_s[i : i + 1, lo:] = top
            weights.append(jnp.exp2((s - top) * e).astype(BF))
            keeps.append(jnp.exp2((old - top) * e))
        for i in range(kb):
            values = jnp.concatenate([v_s[here, _head(i)].T, ones], axis=0)
            mix_s[i, :, lo:] = mix_s[i, :, lo:] * keeps[i] + _dot(values, weights[i])

    lax.fori_loop(0, iq, lambda j, _: block(j * bq, bq, 0, False), None)
    for lo in range(0, bq, STEP):
        block(iq * bq + lo, STEP, lo, True)
    for i in range(kb):
        top, total = top_s[i : i + 1, :], mix_s[i, HEAD : HEAD + 1, :]
        o_ref[:, _head(i)] = (mix_s[i, :HEAD, :] * (1 / total)).T.astype(BF)
        lse_ref[i : i + 1, :] = top * scale + jnp.log(total)
    if joined:
        rest[7][...] = (_dot(before[...], wo_ref[:cols, :]) + _dot(o_ref[...], wo_ref[cols:, :])).astype(BF)


def heads(place, a, own, other, cos, sin, part, before=None, wo=None, bq=1024, rows=512):
    tokens, d = a.shape
    cols = other.shape[1] // 3
    kb = cols // HEAD
    some = lambda wide: pl.BlockSpec((bq, wide), lambda n, p: (n, 0))
    mine = pl.BlockSpec((d // 2, cols), lambda n, p: (0, 2 * p[0] + part))
    whole = lambda t: pl.BlockSpec(t.shape, lambda n, p: (0, 0))
    joined = before is not None
    q, k, v, o, lse, *product = pl.pallas_call(
        functools.partial(_heads, kb=kb, bq=bq, rows=rows, scale=HEAD**-0.5, joined=joined),
        grid_spec=pltpu.PrefetchScalarGridSpec(
            num_scalar_prefetch=1,
            grid=(tokens // bq,),
            in_specs=[some(d), *[mine] * 3, whole(other), some(HEAD), some(HEAD), *([some(cols), whole(wo)] if joined else [])],
            out_specs=[*[some(cols)] * 4, pl.BlockSpec((kb, bq), lambda n, p: (0, n)), *([some(d)] if joined else [])],
            scratch_shapes=[pltpu.VMEM((d, 3 * cols), BF), pltpu.VMEM((tokens, cols), BF), pltpu.VMEM((tokens, cols), BF), pltpu.VMEM((kb, bq), F32),
                            pltpu.VMEM((kb, HEAD + 8, bq), F32)],
        ),
        out_shape=[*[jax.ShapeDtypeStruct((tokens, cols), BF)] * 4, jax.ShapeDtypeStruct((kb, tokens), F32),
                   *([jax.ShapeDtypeStruct((tokens, d), BF)] if joined else [])],
        compiler_params=_params("arbitrary"),
        cost_estimate=pl.CostEstimate(flops=6 * tokens * d * cols + 8 * cols * tokens * tokens, transcendentals=kb * tokens * tokens,
                                      bytes_accessed=2 * (tokens * d + 3 * d * cols + 4 * tokens * cols)),
        name="heads",
    )(place, a, *own, other, cos, sin, *([before, wo] if joined else []))
    return (q, k, v), (o, lse), *product


def _attend_bwd(q_ref, k_ref, v_ref, o_ref, lse_ref, d_ref, wo_ref, cq_ref, sq_ref, cos_ref, sin_ref, dq_ref, dk_ref, dv_ref, do_ref, dq_s, dk_s, dv_s, *, kb, bq, scale):
    iq = pl.program_id(0)
    e = scale * LOG2E

    @pl.when(iq == 0)
    def _():
        dk_s[...] = jnp.zeros_like(dk_s)
        dv_s[...] = jnp.zeros_like(dv_s)

    dq_s[...] = jnp.zeros_like(dq_s)
    do_ref[...] = _dot(d_ref[...], wo_ref[...], 1, 1).astype(BF)
    lses = [lse_ref[i : i + 1, :] * LOG2E for i in range(kb)]
    deltas = [(do_ref[:, _head(i)].astype(F32) * o_ref[:, _head(i)].astype(F32)).T.sum(axis=0, keepdims=True) for i in range(kb)]

    def block(start, size, lo, masked):
        here = pl.ds(pl.multiple_of(start, size), size)
        scores = [_dot(k_ref[here, _head(i)], q_ref[lo:, _head(i)], 1, 1) for i in range(kb)]
        dps = [_dot(v_ref[here, _head(i)], do_ref[lo:, _head(i)], 1, 1) for i in range(kb)]
        ok = _below(size, bq - lo) if masked else None
        for i in range(kb):
            p = jnp.exp2(scores[i] * e - lses[i][:, lo:])
            if masked:
                p = jnp.where(ok, p, 0.0)
            ds = (p * (dps[i] - deltas[i][:, lo:])).astype(BF)
            dv_s[i, here, :] += _dot(p.astype(BF), do_ref[lo:, _head(i)])
            dk_s[i, here, :] += _dot(ds, q_ref[lo:, _head(i)])
            dq_s[i, :, lo:] += _dot(k_ref[here, _head(i)].T, ds)

    lax.fori_loop(0, iq, lambda j, _: block(j * bq, bq, 0, False), None)
    for lo in range(0, bq, STEP):
        block(iq * bq + lo, STEP, lo, True)
    for i in range(kb):
        d = (dq_s[i] * scale).T
        dq_ref[:, _head(i)] = (d * cq_ref[...] + pltpu.roll(d * sq_ref[...], HEAD // 2, 1)).astype(BF)

    @pl.when(iq == pl.num_programs(0) - 1)
    def _():
        for i in range(kb):
            def some(n, _):
                here = pl.ds(pl.multiple_of(n * bq, bq), bq)
                d = dk_s[i, here, :] * scale
                dk_ref[here, _head(i)] = (d * cos_ref[here, :] + pltpu.roll(d * sin_ref[here, :], HEAD // 2, 1)).astype(BF)
                dv_ref[here, _head(i)] = dv_s[i, here, :].astype(BF)

            lax.fori_loop(0, dk_ref.shape[0] // bq, some, None)


def attend_bwd(q, k, v, o, lse, d, wo, cos, sin, part, bq=512):
    tokens, cols = q.shape
    kb = lse.shape[0]
    width = d.shape[1]
    some = pl.BlockSpec((bq, cols), lambda n: (n, 0))
    keys = pl.BlockSpec((tokens, cols), lambda n: (0, 0))
    near = pl.BlockSpec((bq, HEAD), lambda n: (n, 0))
    whole = pl.BlockSpec((tokens, HEAD), lambda n: (0, 0))
    return pl.pallas_call(
        functools.partial(_attend_bwd, kb=kb, bq=bq, scale=HEAD**-0.5),
        grid=(tokens // bq,),
        in_specs=[some, keys, keys, some, pl.BlockSpec((kb, bq), lambda n: (0, n)), pl.BlockSpec((bq, width), lambda n: (n, 0)),
                  pl.BlockSpec((cols, width), lambda n: (part, 0)), near, near, whole, whole],
        out_specs=[some, keys, keys],
        out_shape=[jax.ShapeDtypeStruct(q.shape, BF)] * 3,
        scratch_shapes=[pltpu.VMEM((bq, cols), BF), pltpu.VMEM((kb, HEAD, bq), F32), pltpu.VMEM((kb, tokens, HEAD), F32), pltpu.VMEM((kb, tokens, HEAD), F32)],
        compiler_params=_params("arbitrary"),
        cost_estimate=pl.CostEstimate(flops=16 * cols * tokens * tokens, transcendentals=kb * tokens * tokens, bytes_accessed=16 * tokens * cols),
        name="attend_bwd",
    )(q, k, v, o, lse, d, wo, cos, sin, cos, sin)


def _mlp(place_ref, b_ref, dy_ref, go, uo, gr, ur, dn_ref, *rest, rows, given, begun):
    sums, rest = (rest[:4], rest[4:]) if given else (None, rest)
    db_in, rest = (rest[0], rest[1:]) if begun else (None, rest)
    db_ref, dg_ref, du_ref, dd_ref, dother_ref, gate_s, up_s, dg_s, du_s, dd_s, db_s = rest
    n, place = pl.program_id(0), place_ref[0]
    tokens, d = b_ref.shape
    half = d // 2
    mine, theirs = pl.ds(pl.multiple_of(place * half, half), half), pl.ds(pl.multiple_of((1 - place) * half, half), half)

    @pl.when(n == 0)
    def _():
        db_s[...] = db_in[...] if begun else jnp.zeros_like(db_s)

    dg_s[...] = jnp.zeros_like(dg_s)
    du_s[...] = jnp.zeros_like(du_s)
    dd_s[...] = sums[2][...] if given else jnp.zeros_like(dd_s)
    _whole(gate_s, go[...], gr[...], place)
    _whole(up_s, uo[...], ur[...], place)
    gate_t, up_t = gate_s[...].T, up_s[...].T

    def first(m):
        here = pl.ds(m * rows, rows)
        b, dy = b_ref[here, :], dy_ref[here, :]
        g = _dot(gate_t, b, 1, 1)
        u = _dot(up_t, b, 1, 1)
        dh = _dot(dn_ref[...], dy, 1, 1).astype(BF).astype(F32)
        s = 0.5 * jnp.tanh(0.5 * g) + 0.5
        silu = g * s
        return (silu * u).astype(BF), (dh * u * (s + silu * (1 - s))).astype(BF), (dh * silu).astype(BF)

    def second(m, hidden, dg, du):
        here = pl.ds(m * rows, rows)
        b, dy = b_ref[here, :], dy_ref[here, :]
        dd_s[...] += _dot(hidden, dy)
        dg_s[...] += _dot(dg, b)
        du_s[...] += _dot(du, b)
        db_s[:, here] += _dot(gate_s[...], dg) + _dot(up_s[...], du)

    now = first(0)
    for m in range(tokens // rows):
        then = first(m + 1) if m + 1 < tokens // rows else None
        second(m, *now)
        now = then

    for i, (s, out) in enumerate(((dg_s, dg_ref), (du_s, du_ref))):
        t = s[...].T
        s_own = jnp.where(place == 0, t[:half], t[half:])
        s_other = jnp.where(place == 0, t[half:], t[:half])
        out[...] = ((s_own + sums[i][...]) if given else s_own).astype(out.dtype)
        dother_ref[i] = ((s_other + sums[3][i]) if given else s_other).astype(dother_ref.dtype)
    dd_ref[...] = dd_s[...].astype(dd_ref.dtype)

    @pl.when(n == pl.num_programs(0) - 1)
    def _():
        db_ref[...] = db_s[...].T.astype(BF) if begun else db_s[...]


def mlp(place, b, dy, gate, up, other, down, part, sums=None, db=None, results=None, units=512, rows=512):
    tokens, d = b.shape
    hidden = down.shape[0] // 2
    steps = hidden // units
    final = sums is not None
    kind = BF if final else F32
    given = [*(sums or []), *([db] if db is not None else [])]
    kept = list(results) if results is not None else []
    whole = pl.BlockSpec((tokens, d), lambda n, p: (0, 0))
    whole_t = pl.BlockSpec((d, tokens), lambda n, p: (0, 0))
    own = pl.BlockSpec((d // 2, units), lambda n, p: (0, (2 * p[0] + part) * steps + n))
    got = [pl.BlockSpec((d // 2, units), functools.partial(lambda i, n, p: (0, i * steps + n), i)) for i in range(2)]
    w = pl.BlockSpec((d // 2, units), lambda n, p: (0, n))
    w2 = pl.BlockSpec((2, d // 2, units), lambda n, p: (0, 0, n))
    wd = pl.BlockSpec((units, d), lambda n, p: (n, 0))
    wd_in = pl.BlockSpec((units, d), lambda n, p: (part * steps + n, 0))
    shape = jax.ShapeDtypeStruct
    full = gate.shape if final else (d // 2, hidden)
    first = 8 + len(given)

    def kernel(*refs):
        _mlp(*refs[:first], *refs[first + len(kept) :], rows=rows, given=final, begun=db is not None)

    out, *dw = pl.pallas_call(
        kernel,
        grid_spec=pltpu.PrefetchScalarGridSpec(
            num_scalar_prefetch=1,
            grid=(steps,),
            in_specs=[whole, whole, own, own, *got, wd_in, *([w, w, wd, w2] if final else []), *([whole_t] if db is not None else []),
                      *[pl.BlockSpec(memory_space=pl.ANY)] * len(kept)],
            out_specs=[whole if db is not None else whole_t, *([own, own, wd_in] if final else [w, w, wd]), w2],
            scratch_shapes=[pltpu.VMEM((d, units), BF)] * 2 + [pltpu.VMEM((units, d), F32)] * 3 + [pltpu.VMEM((d, tokens), F32)],
        ),
        out_shape=[shape((tokens, d), BF) if db is not None else shape((d, tokens), F32), shape(full, kind), shape(full, kind),
                   shape((2 * hidden if final else hidden, d), kind), shape((2, d // 2, hidden), kind)],
        input_output_aliases={first + i: 1 + i for i in range(len(kept))},
        compiler_params=_params("arbitrary"),
        cost_estimate=pl.CostEstimate(flops=16 * tokens * d * hidden, transcendentals=tokens * hidden, bytes_accessed=30 * d * hidden),
        name="mlp",
    )(place, b, dy, gate, up, other, other, down, *given, *kept)
    return out, dw


def _states_bwd(place_ref, *refs):
    ds, (qo, ko, vo), others, da_ref, w_s = refs[:6], refs[6:9], refs[9:11], refs[11], refs[12]
    cols = ds[0].shape[1]

    @pl.when(pl.program_id(0) == 0)
    def _():
        for h in range(2):
            for i, own in enumerate((qo, ko, vo)):
                part = slice((3 * h + i) * cols, (3 * h + i + 1) * cols)
                _whole(w_s.at[:, part], own[:, h * cols : (h + 1) * cols], others[h][:, i * cols : (i + 1) * cols], place_ref[0])

    da_ref[...] = sum(_dot(t[...], w_s[:, n * cols : (n + 1) * cols], 1, 1) for n, t in enumerate(ds)).astype(BF)


def states_bwd(place, ds, own, others, rows=512):
    tokens, cols = ds[0].shape
    d = 2 * own[0].shape[0]
    some = lambda wide: pl.BlockSpec((rows, wide), lambda n, p: (n, 0))
    mine = pl.BlockSpec((d // 2, 2 * cols), lambda n, p: (0, p[0]))
    whole = pl.BlockSpec(others[0].shape, lambda n, p: (0, 0))
    return pl.pallas_call(
        _states_bwd,
        grid_spec=pltpu.PrefetchScalarGridSpec(
            num_scalar_prefetch=1,
            grid=(tokens // rows,),
            in_specs=[*[some(cols)] * 6, *[mine] * 3, whole, whole],
            out_specs=some(d),
            scratch_shapes=[pltpu.VMEM((d, 6 * cols), BF)],
        ),
        out_shape=jax.ShapeDtypeStruct((tokens, d), BF),
        compiler_params=_params("arbitrary"),
        cost_estimate=pl.CostEstimate(flops=12 * tokens * d * cols, transcendentals=0, bytes_accessed=2 * (tokens * d + 6 * d * cols + 6 * tokens * cols)),
        name="states_bwd",
    )(place, *ds, *own, *others)


def _weights_bwd(place_ref, a_ref, dq_ref, dk_ref, dv_ref, *rest, given):
    sums, rest = (rest[:4], rest[4:]) if given else (None, rest)
    outs, dother_ref, accs = rest[:3], rest[3], rest[4:]
    n, place = pl.program_id(0), place_ref[0]
    half, cols = a_ref.shape[1] // 2, dq_ref.shape[1]
    mine, theirs = pl.ds(pl.multiple_of(place * half, half), half), pl.ds(pl.multiple_of((1 - place) * half, half), half)
    part = [slice(i * cols, (i + 1) * cols) for i in range(3)]

    @pl.when(n == 0)
    def _():
        for i, s in enumerate(accs):
            if given:
                s[mine, :] = sums[i][...]
                s[theirs, :] = sums[3][:, part[i]]
            else:
                s[...] = jnp.zeros_like(s)

    a_t = a_ref[...].T
    for s, t in zip(accs, (dq_ref, dk_ref, dv_ref)):
        s[...] += _dot(a_t, t[...])

    @pl.when(n == pl.num_programs(0) - 1)
    def _():
        for i, s in enumerate(accs):
            outs[i][...] = s[mine, :].astype(outs[i].dtype)
            dother_ref[:, part[i]] = s[theirs, :].astype(dother_ref.dtype)


def weights_bwd(place, a, ds, part, sums=None, results=None, rows=1024):
    tokens, d = a.shape
    cols = ds[0].shape[1]
    final = sums is not None
    kind = BF if final else F32
    given = list(sums) if final else []
    kept = list(results) if results is not None else []
    some = lambda wide: pl.BlockSpec((rows, wide), lambda n, p: (n, 0))
    mine = pl.BlockSpec((d // 2, cols), lambda n, p: (0, 2 * p[0] + part))
    w = pl.BlockSpec((d // 2, cols), lambda n, p: (0, 0))
    w3 = pl.BlockSpec((d // 2, 3 * cols), lambda n, p: (0, 0))
    shape = jax.ShapeDtypeStruct
    full = (d // 2, 4 * cols) if final else (d // 2, cols)
    first = 5 + len(given)

    def kernel(*refs):
        _weights_bwd(*refs[:first], *refs[first + len(kept) :], given=final)

    return pl.pallas_call(
        kernel,
        grid_spec=pltpu.PrefetchScalarGridSpec(
            num_scalar_prefetch=1,
            grid=(tokens // rows,),
            in_specs=[some(d), *[some(cols)] * 3, *([w, w, w, w3] if final else []), *[pl.BlockSpec(memory_space=pl.ANY)] * len(kept)],
            out_specs=[*[mine if final else w] * 3, w3],
            scratch_shapes=[pltpu.VMEM((d, cols), F32)] * 3,
        ),
        out_shape=[*[shape(full, kind)] * 3, shape((d // 2, 3 * cols), kind)],
        input_output_aliases={first + i: i for i in range(len(kept))},
        compiler_params=_params("arbitrary"),
        cost_estimate=pl.CostEstimate(flops=6 * tokens * d * cols, transcendentals=0, bytes_accessed=2 * (tokens * d + 6 * d * cols + 3 * tokens * cols)),
        name="weights_bwd",
    )(place, a, *ds, *given, *kept)


def normed(h):
    wide = h.astype(F32)
    scale = lax.rsqrt(jnp.mean(wide**2, -1, keepdims=True) + 1e-6)
    return (wide * scale).astype(BF)


def tables(tokens):
    half = HEAD // 2
    angle = jnp.arange(tokens, dtype=F32)[:, None] * THETA ** (-jnp.arange(half, dtype=F32) / half)
    cos, sin = jnp.cos(angle), jnp.sin(angle)
    return jnp.concatenate([cos, cos], 1), jnp.concatenate([-sin, sin], 1)


def after(t, *those):
    return lax.optimization_barrier((t, *those))[0]


def solution(mesh):
    swap = [(0, 1), (1, 0)]
    everyone = ("tp", "dp")

    def step(x, dy, wq, wk, wv, wo, wg, wu, wd):
        p = lax.axis_index("dp")
        place = p.astype(jnp.int32)[None]
        x, dy = x[0], dy[0]
        tokens = x.shape[0] * mesh.shape["tp"]

        def halves(t, axis, n):
            size = t.shape[axis] // 2
            return lax.dynamic_slice_in_dim(t, n * size, size, axis)

        def by_place(mine, theirs):
            return jnp.where(p == 0, mine, theirs), jnp.where(p == 0, theirs, mine)

        def runs(t, *those):
            return by_place(halves(t, 0, p), after(lax.ppermute(halves(t, 0, 1 - p), "dp", swap), *those))

        def gather(t):
            return lax.all_gather(t, everyone, axis=0, tiled=True)

        def collect(part):
            return lax.psum_scatter(part, everyone, scatter_dimension=0, tiled=True)

        def plus(t, more):
            return (t.astype(F32) + more.astype(F32)).astype(BF)

        def to_send(ws, part):
            size = ws[0].shape[1] // 4
            return jnp.concatenate([lax.dynamic_slice_in_dim(w, (2 * (1 - p) + part) * size, size, 1) for w in ws], 1)

        own, own2 = (wq, wk, wv), (wg, wu)
        send = [to_send(own, n) for n in (0, 1)]
        send2 = [to_send(own2, n) for n in (0, 1)]
        xs = runs(x, *send)
        norms, backs = zip(*(jax.vjp(normed, t) for t in xs))
        a = [gather(t) for t in norms]
        other = [lax.ppermute(send[0], "dp", swap)]
        other.append(lax.ppermute(after(send[1], a[0]), "dp", swap))
        other2 = []
        for n in (0, 1):
            other2.append(lax.ppermute(after(send2[n], a[0]), "dp", swap))
        cos, sin = tables(tokens)

        def half_heads(a, n, *more):
            return heads(place, a, own, other[n], cos, sin, n, *more)

        t00, o00 = half_heads(after(a[0], norms[1]), 0)
        dys = runs(dy, o00[0])
        t01, o01, h0 = half_heads(after(a[0], *dys), 1, o00[0], wo)
        dy_all = [gather(dys[0])]
        h0 = collect(after(h0, dy_all[0], a[1]))
        dy_all.append(gather(after(dys[1], h0)))
        t10, o10 = half_heads(after(a[1], o01[0]), 0)
        h0 = plus(xs[0], after(h0, o10[0]))
        b0, back0 = jax.vjp(normed, h0)
        t11, o11, h1 = half_heads(after(a[1], b0), 1, o10[0], wo)
        b0 = gather(b0)
        h1 = collect(h1)
        db0, w0a = mlp(place, b0, dy_all[0], wg, wu, other2[0], wd, 0)
        h1 = plus(xs[1], after(h1, db0))
        b1, back1 = jax.vjp(normed, h1)
        db0, w0b = mlp(place, after(b0, b1), dy_all[0], wg, wu, other2[1], wd, 1, None, db0)
        b1 = gather(b1)
        db0 = collect(db0)
        db1, w1a = mlp(place, b1, dy_all[1], wg, wu, other2[0], wd, 0, w0a)
        ga = lax.ppermute(w1a[3], "dp", swap)
        dh0 = plus(dys[0], back0(after(db0, db1))[0])
        db1, w1b = mlp(place, after(b1, dh0), dy_all[1], wg, wu, other2[1], wd, 1, w0b, db1, w1a[:3])
        d0 = gather(dh0)
        gb = lax.ppermute(w1b[3], "dp", swap)
        db1 = collect(db1)

        def heads_back(t, o, d, n):
            return attend_bwd(*t, *o, d, wo, cos, sin, n)

        ds0 = heads_back(t00, o00, d0, 0)
        dh1 = plus(dys[1], back1(after(db1, ds0[0]))[0])
        ds1 = heads_back((after(t01[0], dh1), *t01[1:]), o01, d0, 1)
        d1 = gather(dh1)
        da0 = collect(after(states_bwd(place, [*ds0, *ds1], own, other), d1))
        s0, s1 = (weights_bwd(place, a[0], t, n) for n, t in enumerate((ds0, ds1)))
        ds0 = heads_back(t10, o10, after(d1, s0[3], s1[3]), 0)
        s0 = weights_bwd(place, a[1], ds0, 0, s0)
        g0 = lax.ppermute(s0[3], "dp", swap)
        ds1 = heads_back((after(t11[0], s0[3]), *t11[1:]), o11, d1, 1)
        da1 = states_bwd(place, [*ds0, *ds1], own, other)
        s1 = weights_bwd(place, after(a[1], da1), ds1, 1, s1, s0[:3])
        da1 = collect(da1)
        g1 = lax.ppermute(s1[3], "dp", swap)
        dx0 = plus(dh0, backs[0](da0)[0])
        dx1 = plus(dh1, backs[1](da1)[0])
        mine, theirs = by_place(dx0, dx1)
        theirs = lax.ppermute(theirs, "dp", swap)
        dx = jnp.concatenate(by_place(mine, theirs), 0)
        dwo = jnp.concatenate([(_dot(m[0], d0, 0, 0) + _dot(n[0], d1, 0, 0)).astype(BF) for m, n in ((o00, o10), (o01, o11))], 0)

        def with_other(full, *got):
            size = got[0].shape[1]
            for n, t in enumerate(got):
                full = lax.dynamic_update_slice(full, t, (0, (2 * (1 - p) + n) * size))
            return full

        cols = g0.shape[1] // 3
        dw = [with_other(s1[i], *(g[:, i * cols : (i + 1) * cols] for g in (g0, g1))) for i in range(3)]
        ga, gb = after(ga, s1[3]), after(gb, s1[3])
        dwg, dwu = (with_other(w1b[i], ga[i], gb[i]) for i in range(2))
        return (dx[None], *dw, dwo, dwg, dwu, w1b[2])

    states, by_columns, by_rows = P("dp", "tp", None), P("dp", "tp"), P(("tp", "dp"), None)
    weights = (by_columns, by_columns, by_columns, by_rows, by_columns, by_columns, by_rows)
    return jax.shard_map(step, mesh=mesh, in_specs=(states, states, *weights), out_specs=(states, *weights), check_vma=False)
```

```python
import functools

import jax
import jax.numpy as jnp
from jax import lax
from jax.experimental import pallas as pl
from jax.experimental.pallas import tpu as pltpu
from jax.sharding import PartitionSpec as P

HEAD = 128
THETA = 10000
NEG = -1e30
HIDDEN = 2 * NEG
LOG2E = 1.4426950408889634
VMEM = 60 * 2**20
STEP = 256
BF, F32 = jnp.bfloat16, jnp.float32


def _dot(a, b, ca=1, cb=0):
    return lax.dot_general(a, b, (((ca,), (cb,)), ((), ())), preferred_element_type=F32)


def _params(*kinds):
    return pltpu.CompilerParams(dimension_semantics=kinds, vmem_limit_bytes=VMEM)


def _head(i):
    return slice(i * HEAD, (i + 1) * HEAD)


def _whole(scratch, own, other, place):
    half = own.shape[0]
    scratch[pl.ds(pl.multiple_of(place * half, half), half), :] = own
    scratch[pl.ds(pl.multiple_of((1 - place) * half, half), half), :] = other


def _below(bk, bq):
    return lax.broadcasted_iota(jnp.int32, (bk, bq), 1) >= lax.broadcasted_iota(jnp.int32, (bk, bq), 0)


def _heads(place_ref, a_ref, qo, ko, vo, other, cos_ref, sin_ref, *rest, kb, bq, rows, scale, joined):
    before, wo_ref = rest[:2] if joined else (None, None)
    q_ref, k_ref, v_ref, o_ref, lse_ref = rest[2:7] if joined else rest[:5]
    w_s, k_s, v_s, top_s, mix_s = rest[-5:]
    iq = pl.program_id(0)
    cols = kb * HEAD

    @pl.when(iq == 0)
    def _():
        for i, own in enumerate((qo, ko, vo)):
            part = slice(i * cols, (i + 1) * cols)
            _whole(w_s.at[:, part], own[...], other[:, part], place_ref[0])

    def some(n, _):
        here = pl.ds(pl.multiple_of(n * rows, rows), rows)
        there = pl.ds(pl.multiple_of(iq * bq + n * rows, rows), rows)
        cos, sin = cos_ref[here, :], sin_ref[here, :]
        for i, out in enumerate((q_ref, k_ref, v_ref)):
            t = _dot(a_ref[here, :], w_s[:, i * cols : (i + 1) * cols]).astype(BF)
            for h in range(kb):
                u = t[:, _head(h)]
                if i < 2:
                    u = u.astype(F32)
                    u = (u * cos + pltpu.roll(u, HEAD // 2, 1) * sin).astype(BF)
                out[here, _head(h)] = u
                if i > 0:
                    (k_s if i == 1 else v_s)[there, _head(h)] = u

    lax.fori_loop(0, bq // rows, some, None)
    e = scale * LOG2E
    top_s[...] = jnp.full(top_s.shape, NEG, F32)
    mix_s[...] = jnp.zeros(mix_s.shape, F32)

    def block(start, size, lo, masked):
        here = pl.ds(pl.multiple_of(start, size), size)
        scores = [_dot(k_s[here, _head(i)], q_ref[lo:, _head(i)], 1, 1) for i in range(kb)]
        ok = _below(size, bq - lo) if masked else None
        ones = jnp.ones((8, size), BF)
        weights, keeps = [], []
        for i, s in enumerate(scores):
            if masked:
                s = jnp.where(ok, s, HIDDEN)
            old = top_s[i : i + 1, lo:]
            top = jnp.maximum(old, s.max(axis=0, keepdims=True))
            top_s[i : i + 1, lo:] = top
            weights.append(jnp.exp2((s - top) * e).astype(BF))
            keeps.append(jnp.exp2((old - top) * e))
        for i in range(kb):
            values = jnp.concatenate([v_s[here, _head(i)].T, ones], axis=0)
            mix_s[i, :, lo:] = mix_s[i, :, lo:] * keeps[i] + _dot(values, weights[i])

    lax.fori_loop(0, iq, lambda j, _: block(j * bq, bq, 0, False), None)
    for lo in range(0, bq, STEP):
        block(iq * bq + lo, STEP, lo, True)
    for i in range(kb):
        top, total = top_s[i : i + 1, :], mix_s[i, HEAD : HEAD + 1, :]
        o_ref[:, _head(i)] = (mix_s[i, :HEAD, :] * (1 / total)).T.astype(BF)
        lse_ref[i : i + 1, :] = top * scale + jnp.log(total)
    if joined:
        rest[7][...] = (_dot(before[...], wo_ref[:cols, :]) + _dot(o_ref[...], wo_ref[cols:, :])).astype(BF)


def heads(place, a, own, other, cos, sin, part, before=None, wo=None, bq=1024, rows=512):
    tokens, d = a.shape[0], 2 * other.shape[0]
    cols = other.shape[1] // 3
    kb = cols // HEAD
    some = lambda wide: pl.BlockSpec((bq, wide), lambda n, p: (n, 0))
    mine = pl.BlockSpec((d // 2, cols), lambda n, p: (0, 2 * p[0] + part))
    whole = lambda t: pl.BlockSpec(t.shape, lambda n, p: (0, 0))
    joined = before is not None
    q, k, v, o, lse, *product = pl.pallas_call(
        functools.partial(_heads, kb=kb, bq=bq, rows=rows, scale=HEAD**-0.5, joined=joined),
        grid_spec=pltpu.PrefetchScalarGridSpec(
            num_scalar_prefetch=1,
            grid=(tokens // bq,),
            in_specs=[some(d), *[mine] * 3, whole(other), some(HEAD), some(HEAD), *([some(cols), whole(wo)] if joined else [])],
            out_specs=[*[some(cols)] * 4, pl.BlockSpec((kb, bq), lambda n, p: (0, n)), *([some(d)] if joined else [])],
            scratch_shapes=[pltpu.VMEM((d, 3 * cols), BF), pltpu.VMEM((tokens, cols), BF), pltpu.VMEM((tokens, cols), BF), pltpu.VMEM((kb, bq), F32),
                            pltpu.VMEM((kb, HEAD + 8, bq), F32)],
        ),
        out_shape=[*[jax.ShapeDtypeStruct((tokens, cols), BF)] * 4, jax.ShapeDtypeStruct((kb, tokens), F32),
                   *([jax.ShapeDtypeStruct((tokens, d), BF)] if joined else [])],
        compiler_params=_params("arbitrary"),
        cost_estimate=pl.CostEstimate(flops=6 * tokens * d * cols + 8 * cols * tokens * tokens, transcendentals=kb * tokens * tokens,
                                      bytes_accessed=2 * (tokens * d + 3 * d * cols + 4 * tokens * cols)),
        name="heads",
    )(place, a, *own, other, cos, sin, *([before, wo] if joined else []))
    return (q, k, v), (o, lse), *product


def _attend_bwd(q_ref, k_ref, v_ref, o_ref, lse_ref, d_ref, wo_ref, cq_ref, sq_ref, cos_ref, sin_ref, dq_ref, dk_ref, dv_ref, do_ref, dq_s, dk_s, dv_s, *, kb, bq, scale):
    iq = pl.program_id(0)
    e = scale * LOG2E

    @pl.when(iq == 0)
    def _():
        dk_s[...] = jnp.zeros_like(dk_s)
        dv_s[...] = jnp.zeros_like(dv_s)

    dq_s[...] = jnp.zeros_like(dq_s)
    do_ref[...] = _dot(d_ref[...], wo_ref[...], 1, 1).astype(BF)
    lses = [lse_ref[i : i + 1, :] * LOG2E for i in range(kb)]
    deltas = [(do_ref[:, _head(i)].astype(F32) * o_ref[:, _head(i)].astype(F32)).T.sum(axis=0, keepdims=True) for i in range(kb)]

    def block(start, size, lo, masked):
        here = pl.ds(pl.multiple_of(start, size), size)
        scores = [_dot(k_ref[here, _head(i)], q_ref[lo:, _head(i)], 1, 1) for i in range(kb)]
        dps = [_dot(v_ref[here, _head(i)], do_ref[lo:, _head(i)], 1, 1) for i in range(kb)]
        ok = _below(size, bq - lo) if masked else None
        for i in range(kb):
            p = jnp.exp2(scores[i] * e - lses[i][:, lo:])
            if masked:
                p = jnp.where(ok, p, 0.0)
            ds = (p * (dps[i] - deltas[i][:, lo:])).astype(BF)
            dv_s[i, here, :] += _dot(p.astype(BF), do_ref[lo:, _head(i)])
            dk_s[i, here, :] += _dot(ds, q_ref[lo:, _head(i)])
            dq_s[i, :, lo:] += _dot(k_ref[here, _head(i)].T, ds)

    lax.fori_loop(0, iq, lambda j, _: block(j * bq, bq, 0, False), None)
    for lo in range(0, bq, STEP):
        block(iq * bq + lo, STEP, lo, True)
    for i in range(kb):
        d = (dq_s[i] * scale).T
        dq_ref[:, _head(i)] = (d * cq_ref[...] + pltpu.roll(d * sq_ref[...], HEAD // 2, 1)).astype(BF)

    @pl.when(iq == pl.num_programs(0) - 1)
    def _():
        for i in range(kb):
            def some(n, _):
                here = pl.ds(pl.multiple_of(n * bq, bq), bq)
                d = dk_s[i, here, :] * scale
                dk_ref[here, _head(i)] = (d * cos_ref[here, :] + pltpu.roll(d * sin_ref[here, :], HEAD // 2, 1)).astype(BF)
                dv_ref[here, _head(i)] = dv_s[i, here, :].astype(BF)

            lax.fori_loop(0, dk_ref.shape[0] // bq, some, None)


def attend_bwd(q, k, v, o, lse, d, wo, cos, sin, part, bq=512):
    tokens, cols = q.shape
    kb = lse.shape[0]
    width = d.shape[1]
    some = pl.BlockSpec((bq, cols), lambda n: (n, 0))
    keys = pl.BlockSpec((tokens, cols), lambda n: (0, 0))
    near = pl.BlockSpec((bq, HEAD), lambda n: (n, 0))
    whole = pl.BlockSpec((tokens, HEAD), lambda n: (0, 0))
    return pl.pallas_call(
        functools.partial(_attend_bwd, kb=kb, bq=bq, scale=HEAD**-0.5),
        grid=(tokens // bq,),
        in_specs=[some, keys, keys, some, pl.BlockSpec((kb, bq), lambda n: (0, n)), pl.BlockSpec((bq, width), lambda n: (n, 0)),
                  pl.BlockSpec((cols, width), lambda n: (part, 0)), near, near, whole, whole],
        out_specs=[some, keys, keys],
        out_shape=[jax.ShapeDtypeStruct(q.shape, BF)] * 3,
        scratch_shapes=[pltpu.VMEM((bq, cols), BF), pltpu.VMEM((kb, HEAD, bq), F32), pltpu.VMEM((kb, tokens, HEAD), F32), pltpu.VMEM((kb, tokens, HEAD), F32)],
        compiler_params=_params("arbitrary"),
        cost_estimate=pl.CostEstimate(flops=16 * cols * tokens * tokens, transcendentals=kb * tokens * tokens, bytes_accessed=16 * tokens * cols),
        name="attend_bwd",
    )(q, k, v, o, lse, d, wo, cos, sin, cos, sin)


def _mlp(place_ref, b_ref, dy_ref, go, uo, gr, ur, dn_ref, *rest, rows, given, begun):
    sums, rest = (rest[:4], rest[4:]) if given else (None, rest)
    db_in, rest = (rest[0], rest[1:]) if begun else (None, rest)
    db_ref, dg_ref, du_ref, dd_ref, dother_ref, gate_s, up_s, dg_s, du_s, dd_s, db_s = rest
    n, place = pl.program_id(0), place_ref[0]
    tokens, d = b_ref.shape
    half = d // 2
    mine, theirs = pl.ds(pl.multiple_of(place * half, half), half), pl.ds(pl.multiple_of((1 - place) * half, half), half)

    @pl.when(n == 0)
    def _():
        db_s[...] = db_in[...] if begun else jnp.zeros_like(db_s)

    dg_s[...] = jnp.zeros_like(dg_s)
    du_s[...] = jnp.zeros_like(du_s)
    dd_s[...] = sums[2][...] if given else jnp.zeros_like(dd_s)
    _whole(gate_s, go[...], gr[...], place)
    _whole(up_s, uo[...], ur[...], place)
    gate_t, up_t = gate_s[...].T, up_s[...].T

    def first(m):
        here = pl.ds(m * rows, rows)
        b, dy = b_ref[here, :], dy_ref[here, :]
        g = _dot(gate_t, b, 1, 1)
        u = _dot(up_t, b, 1, 1)
        dh = _dot(dn_ref[...], dy, 1, 1).astype(BF).astype(F32)
        s = 0.5 * jnp.tanh(0.5 * g) + 0.5
        silu = g * s
        return (silu * u).astype(BF), (dh * u * (s + silu * (1 - s))).astype(BF), (dh * silu).astype(BF)

    def second(m, hidden, dg, du):
        here = pl.ds(m * rows, rows)
        b, dy = b_ref[here, :], dy_ref[here, :]
        dd_s[...] += _dot(hidden, dy)
        dg_s[...] += _dot(dg, b)
        du_s[...] += _dot(du, b)
        db_s[:, here] += _dot(gate_s[...], dg) + _dot(up_s[...], du)

    now = first(0)
    for m in range(tokens // rows):
        then = first(m + 1) if m + 1 < tokens // rows else None
        second(m, *now)
        now = then

    for i, (s, out) in enumerate(((dg_s, dg_ref), (du_s, du_ref))):
        t = s[...].T
        s_own = jnp.where(place == 0, t[:half], t[half:])
        s_other = jnp.where(place == 0, t[half:], t[:half])
        out[...] = ((s_own + sums[i][...]) if given else s_own).astype(out.dtype)
        dother_ref[i] = ((s_other + sums[3][i]) if given else s_other).astype(dother_ref.dtype)
    dd_ref[...] = dd_s[...].astype(dd_ref.dtype)

    @pl.when(n == pl.num_programs(0) - 1)
    def _():
        db_ref[...] = db_s[...].T.astype(BF) if begun else db_s[...]


def mlp(place, b, dy, at, gate, up, other, down, part, sums=None, db=None, results=None, units=512, rows=512):
    tokens, d = b.shape
    hidden = down.shape[0] // 2
    steps = hidden // units
    final = sums is not None
    kind = BF if final else F32
    given = [*(sums or []), *([db] if db is not None else [])]
    kept = list(results) if results is not None else []
    whole = pl.BlockSpec((tokens, d), lambda n, p: (0, 0))
    whole_t = pl.BlockSpec((d, tokens), lambda n, p: (0, 0))
    own = pl.BlockSpec((d // 2, units), lambda n, p: (0, (2 * p[0] + part) * steps + n))
    got = [pl.BlockSpec((d // 2, units), functools.partial(lambda i, n, p: (0, i * steps + n), i)) for i in range(2)]
    w = pl.BlockSpec((d // 2, units), lambda n, p: (0, n))
    w2 = pl.BlockSpec((2, d // 2, units), lambda n, p: (0, 0, n))
    wd = pl.BlockSpec((units, d), lambda n, p: (n, 0))
    wd_in = pl.BlockSpec((units, d), lambda n, p: (part * steps + n, 0))
    shape = jax.ShapeDtypeStruct
    full = gate.shape if final else (d // 2, hidden)
    first = 8 + len(given)

    def kernel(*refs):
        _mlp(*refs[:first], *refs[first + len(kept) :], rows=rows, given=final, begun=db is not None)

    out, *dw = pl.pallas_call(
        kernel,
        grid_spec=pltpu.PrefetchScalarGridSpec(
            num_scalar_prefetch=1,
            grid=(steps,),
            in_specs=[whole, pl.BlockSpec((tokens, d), lambda n, p: (0, at)), own, own, *got, wd_in, *([w, w, wd, w2] if final else []), *([whole_t] if db is not None else []),
                      *[pl.BlockSpec(memory_space=pl.ANY)] * len(kept)],
            out_specs=[whole if db is not None else whole_t, *([own, own, wd_in] if final else [w, w, wd]), w2],
            scratch_shapes=[pltpu.VMEM((d, units), BF)] * 2 + [pltpu.VMEM((units, d), F32)] * 3 + [pltpu.VMEM((d, tokens), F32)],
        ),
        out_shape=[shape((tokens, d), BF) if db is not None else shape((d, tokens), F32), shape(full, kind), shape(full, kind),
                   shape((2 * hidden if final else hidden, d), kind), shape((2, d // 2, hidden), kind)],
        input_output_aliases={first + i: 1 + i for i in range(len(kept))},
        compiler_params=_params("arbitrary"),
        cost_estimate=pl.CostEstimate(flops=16 * tokens * d * hidden, transcendentals=tokens * hidden, bytes_accessed=30 * d * hidden),
        name="mlp",
    )(place, b, dy, gate, up, other, other, down, *given, *kept)
    return out, dw


def _states_bwd(place_ref, *refs, begun, last):
    halves = (len(refs) - 5 - begun) // 4
    ds, (qo, ko, vo), others = refs[: 3 * halves], refs[3 * halves : 3 * halves + 3], refs[3 * halves + 3 : 4 * halves + 3]
    da_ref, w_s = refs[-2:]
    cols = ds[0].shape[1]

    @pl.when(pl.program_id(0) == 0)
    def _():
        for h in range(halves):
            for i, own in enumerate((qo, ko, vo)):
                part = slice((3 * h + i) * cols, (3 * h + i + 1) * cols)
                _whole(w_s.at[:, part], own[:, h * cols : (h + 1) * cols], others[h][:, i * cols : (i + 1) * cols], place_ref[0])

    da = sum(_dot(t[...], w_s[:, n * cols : (n + 1) * cols], 1, 1) for n, t in enumerate(ds))
    if begun:
        da += refs[-3][...]
    da_ref[...] = da.astype(BF) if last else da


def states_bwd(place, ds, own, others, parts=(0, 1), da=None, rows=512):
    tokens, cols = ds[0].shape
    d = 2 * own[0].shape[0]
    last = len(parts) == 2 or da is not None
    some = lambda wide: pl.BlockSpec((rows, wide), lambda n, p: (n, 0))
    mine = pl.BlockSpec((d // 2, len(parts) * cols), (lambda n, p: (0, p[0])) if len(parts) == 2 else (lambda n, p: (0, 2 * p[0] + parts[0])))
    whole = pl.BlockSpec(others[0].shape, lambda n, p: (0, 0))
    given = [] if da is None else [da]
    return pl.pallas_call(
        functools.partial(_states_bwd, begun=len(given), last=last),
        grid_spec=pltpu.PrefetchScalarGridSpec(
            num_scalar_prefetch=1,
            grid=(tokens // rows,),
            in_specs=[*[some(cols)] * len(ds), *[mine] * 3, *[whole] * len(parts), *[some(d)] * len(given)],
            out_specs=some(d),
            scratch_shapes=[pltpu.VMEM((d, 3 * len(parts) * cols), BF)],
        ),
        out_shape=jax.ShapeDtypeStruct((tokens, d), BF if last else F32),
        compiler_params=_params("arbitrary"),
        cost_estimate=pl.CostEstimate(flops=6 * len(parts) * tokens * d * cols, transcendentals=0, bytes_accessed=2 * (tokens * d + 3 * len(parts) * (d + tokens) * cols)),
        name="states_bwd",
    )(place, *ds, *own, *others, *given)


def _weights_bwd(place_ref, a_ref, dq_ref, dk_ref, dv_ref, *rest, given):
    sums, rest = (rest[:4], rest[4:]) if given else (None, rest)
    outs, dother_ref, accs = rest[:3], rest[3], rest[4:]
    n, place = pl.program_id(0), place_ref[0]
    half, cols = a_ref.shape[1] // 2, dq_ref.shape[1]
    mine, theirs = pl.ds(pl.multiple_of(place * half, half), half), pl.ds(pl.multiple_of((1 - place) * half, half), half)
    part = [slice(i * cols, (i + 1) * cols) for i in range(3)]

    @pl.when(n == 0)
    def _():
        for i, s in enumerate(accs):
            if given:
                s[mine, :] = sums[i][...]
                s[theirs, :] = sums[3][:, part[i]]
            else:
                s[...] = jnp.zeros_like(s)

    a_t = a_ref[...].T
    for s, t in zip(accs, (dq_ref, dk_ref, dv_ref)):
        s[...] += _dot(a_t, t[...])

    @pl.when(n == pl.num_programs(0) - 1)
    def _():
        for i, s in enumerate(accs):
            outs[i][...] = s[mine, :].astype(outs[i].dtype)
            dother_ref[:, part[i]] = s[theirs, :].astype(dother_ref.dtype)


def weights_bwd(place, a, ds, d, part, sums=None, results=None, rows=1024):
    tokens, cols = ds[0].shape
    final = sums is not None
    kind = BF if final else F32
    given = list(sums) if final else []
    kept = list(results) if results is not None else []
    some = lambda wide: pl.BlockSpec((rows, wide), lambda n, p: (n, 0))
    mine = pl.BlockSpec((d // 2, cols), lambda n, p: (0, 2 * p[0] + part))
    w = pl.BlockSpec((d // 2, cols), lambda n, p: (0, 0))
    w3 = pl.BlockSpec((d // 2, 3 * cols), lambda n, p: (0, 0))
    shape = jax.ShapeDtypeStruct
    full = (d // 2, 4 * cols) if final else (d // 2, cols)
    first = 5 + len(given)

    def kernel(*refs):
        _weights_bwd(*refs[:first], *refs[first + len(kept) :], given=final)

    return pl.pallas_call(
        kernel,
        grid_spec=pltpu.PrefetchScalarGridSpec(
            num_scalar_prefetch=1,
            grid=(tokens // rows,),
            in_specs=[some(d), *[some(cols)] * 3, *([w, w, w, w3] if final else []), *[pl.BlockSpec(memory_space=pl.ANY)] * len(kept)],
            out_specs=[*[mine if final else w] * 3, w3],
            scratch_shapes=[pltpu.VMEM((d, cols), F32)] * 3,
        ),
        out_shape=[*[shape(full, kind)] * 3, shape((d // 2, 3 * cols), kind)],
        input_output_aliases={first + i: i for i in range(len(kept))},
        compiler_params=_params("arbitrary"),
        cost_estimate=pl.CostEstimate(flops=6 * tokens * d * cols, transcendentals=0, bytes_accessed=2 * (tokens * d + 6 * d * cols + 3 * tokens * cols)),
        name="weights_bwd",
    )(place, a, *ds, *given, *kept)


def normed(h):
    wide = h.astype(F32)
    scale = lax.rsqrt(jnp.mean(wide**2, -1, keepdims=True) + 1e-6)
    return (wide * scale).astype(BF)


def tables(tokens):
    half = HEAD // 2
    angle = jnp.arange(tokens, dtype=F32)[:, None] * THETA ** (-jnp.arange(half, dtype=F32) / half)
    cos, sin = jnp.cos(angle), jnp.sin(angle)
    return jnp.concatenate([cos, cos], 1), jnp.concatenate([-sin, sin], 1)


def after(t, *those):
    return lax.optimization_barrier((t, *those))[0]


def solution(mesh):
    swap = [(0, 1), (1, 0)]
    everyone = ("tp", "dp")

    def step(x, dy, wq, wk, wv, wo, wg, wu, wd):
        p = lax.axis_index("dp")
        place = p.astype(jnp.int32)[None]
        x, dy = x[0], dy[0]
        tokens = x.shape[0] * mesh.shape["tp"]

        def halves(t, axis, n):
            size = t.shape[axis] // 2
            return lax.dynamic_slice_in_dim(t, n * size, size, axis)

        def by_place(mine, theirs):
            return jnp.where(p == 0, mine, theirs), jnp.where(p == 0, theirs, mine)

        def runs(t, *those):
            return by_place(halves(t, 0, p), after(lax.ppermute(halves(t, 0, 1 - p), "dp", swap), *those))

        def gather(t):
            return lax.all_gather(t, everyone, axis=0, tiled=True)

        def collect(part):
            return lax.psum_scatter(part, everyone, scatter_dimension=0, tiled=True)

        def plus(t, more):
            return (t.astype(F32) + more.astype(F32)).astype(BF)

        def to_send(ws, part):
            size = ws[0].shape[1] // 4
            return jnp.concatenate([lax.dynamic_slice_in_dim(w, (2 * (1 - p) + part) * size, size, 1) for w in ws], 1)

        own, own2 = (wq, wk, wv), (wg, wu)
        send = [to_send(own, n) for n in (0, 1)]
        send2 = [to_send(own2, n) for n in (0, 1)]
        xs = runs(x, *send)
        norms, backs = zip(*(jax.vjp(normed, t) for t in xs))
        dys = runs(dy, *send)
        a = [gather(norms[0]), gather(jnp.concatenate([norms[1], dys[0]], 1))]
        other = [lax.ppermute(send[0], "dp", swap)]
        other.append(lax.ppermute(after(send[1], a[0]), "dp", swap))
        other2 = []
        for n in (0, 1):
            other2.append(lax.ppermute(after(send2[n], a[0]), "dp", swap))
        cos, sin = tables(tokens)

        def half_heads(a, n, *more):
            return heads(place, a, own, other[n], cos, sin, n, *more)

        t00, o00 = half_heads(after(a[0], norms[1], dys[0]), 0)
        t01, o01, h0 = half_heads(a[0], 1, o00[0], wo)
        h0 = collect(after(h0, a[1]))
        dy1 = gather(after(dys[1], h0))
        t10, o10 = half_heads(after(a[1], o01[0]), 0)
        h0 = plus(xs[0], after(h0, o10[0]))
        b0, back0 = jax.vjp(normed, h0)
        t11, o11, h1 = half_heads(after(a[1], b0), 1, o10[0], wo)
        b0 = gather(b0)
        h1 = collect(h1)
        db0, w0a = mlp(place, b0, a[1], 1, wg, wu, other2[0], wd, 0)
        h1 = plus(xs[1], after(h1, db0))
        b1, back1 = jax.vjp(normed, h1)
        db0, w0b = mlp(place, after(b0, b1), a[1], 1, wg, wu, other2[1], wd, 1, None, db0)
        b1 = gather(b1)
        db0 = collect(db0)
        db1, w1a = mlp(place, b1, dy1, 0, wg, wu, other2[0], wd, 0, w0a)
        ga = lax.ppermute(w1a[3], "dp", swap)
        dh0 = plus(dys[0], back0(after(db0, db1))[0])
        db1, w1b = mlp(place, after(b1, dh0), dy1, 0, wg, wu, other2[1], wd, 1, w0b, db1, w1a[:3])
        d0 = gather(dh0)
        gb = lax.ppermute(w1b[3], "dp", swap)
        db1 = collect(db1)

        def heads_back(t, o, d, n):
            return attend_bwd(*t, *o, d, wo, cos, sin, n)

        ds0 = heads_back(t00, o00, d0, 0)
        dh1 = plus(dys[1], back1(after(db1, ds0[0]))[0])
        ds1 = heads_back((after(t01[0], dh1), *t01[1:]), o01, d0, 1)
        d1 = gather(dh1)
        da0 = collect(after(states_bwd(place, [*ds0, *ds1], own, other), d1))
        s0, s1 = (weights_bwd(place, a[0], t, x.shape[1], n) for n, t in enumerate((ds0, ds1)))
        ds0 = heads_back(t10, o10, after(d1, s0[3], s1[3]), 0)
        da1 = states_bwd(place, ds0, own, other[:1], (0,))
        s0 = weights_bwd(place, a[1], ds0, x.shape[1], 0, s0)
        g0 = lax.ppermute(s0[3], "dp", swap)
        ds1 = heads_back((after(t11[0], s0[3], da1), *t11[1:]), o11, d1, 1)
        da1 = states_bwd(place, ds1, own, other[1:], (1,), da1)
        s1 = weights_bwd(place, after(a[1], da1), ds1, x.shape[1], 1, s1, s0[:3])
        da1 = collect(da1)
        g1 = lax.ppermute(s1[3], "dp", swap)
        dx0 = plus(dh0, backs[0](da0)[0])
        dx1 = plus(dh1, backs[1](da1)[0])
        mine, theirs = by_place(dx0, dx1)
        theirs = lax.ppermute(theirs, "dp", swap)
        dx = jnp.concatenate(by_place(mine, theirs), 0)
        dwo = jnp.concatenate([(_dot(m[0], d0, 0, 0) + _dot(n[0], d1, 0, 0)).astype(BF) for m, n in ((o00, o10), (o01, o11))], 0)

        def with_other(full, *got):
            size = got[0].shape[1]
            for n, t in enumerate(got):
                full = lax.dynamic_update_slice(full, t, (0, (2 * (1 - p) + n) * size))
            return full

        cols = g0.shape[1] // 3
        dw = [with_other(s1[i], *(g[:, i * cols : (i + 1) * cols] for g in (g0, g1))) for i in range(3)]
        ga, gb = after(ga, s1[3]), after(gb, s1[3])
        dwg, dwu = (with_other(w1b[i], ga[i], gb[i]) for i in range(2))
        return (dx[None], *dw, dwo, dwg, dwu, w1b[2])

    states, by_columns, by_rows = P("dp", "tp", None), P("dp", "tp"), P(("tp", "dp"), None)
    weights = (by_columns, by_columns, by_columns, by_rows, by_columns, by_columns, by_rows)
    return jax.shard_map(step, mesh=mesh, in_specs=(states, states, *weights), out_specs=(states, *weights), check_vma=False)
```

```python
import functools

import jax
import jax.numpy as jnp
from jax import lax
from jax.experimental import pallas as pl
from jax.experimental.pallas import tpu as pltpu
from jax.sharding import PartitionSpec as P

HEAD = 128
THETA = 10000
NEG = -1e30
HIDDEN = 2 * NEG
LOG2E = 1.4426950408889634
VMEM = 60 * 2**20
STEP = 256
BF, F32 = jnp.bfloat16, jnp.float32


def _dot(a, b, ca=1, cb=0):
    return lax.dot_general(a, b, (((ca,), (cb,)), ((), ())), preferred_element_type=F32)


def _params(*kinds):
    return pltpu.CompilerParams(dimension_semantics=kinds, vmem_limit_bytes=VMEM)


def _head(i):
    return slice(i * HEAD, (i + 1) * HEAD)


def _whole(scratch, own, other, place):
    half = own.shape[0]
    scratch[pl.ds(pl.multiple_of(place * half, half), half), :] = own
    scratch[pl.ds(pl.multiple_of((1 - place) * half, half), half), :] = other


def _below(bk, bq):
    return lax.broadcasted_iota(jnp.int32, (bk, bq), 1) >= lax.broadcasted_iota(jnp.int32, (bk, bq), 0)


def _heads(place_ref, a_ref, qo, ko, vo, other, cos_ref, sin_ref, *rest, kb, bq, rows, scale, joined):
    before, wo_ref = rest[:2] if joined else (None, None)
    q_ref, k_ref, v_ref, o_ref, lse_ref = rest[2:7] if joined else rest[:5]
    w_s, k_s, v_s, top_s, mix_s = rest[-5:]
    iq = pl.program_id(0)
    cols = kb * HEAD

    @pl.when(iq == 0)
    def _():
        for i, own in enumerate((qo, ko, vo)):
            part = slice(i * cols, (i + 1) * cols)
            _whole(w_s.at[:, part], own[...], other[:, part], place_ref[0])

    def some(n, _):
        here = pl.ds(pl.multiple_of(n * rows, rows), rows)
        there = pl.ds(pl.multiple_of(iq * bq + n * rows, rows), rows)
        cos, sin = cos_ref[here, :], sin_ref[here, :]
        for i, out in enumerate((q_ref, k_ref, v_ref)):
            t = _dot(a_ref[here, :], w_s[:, i * cols : (i + 1) * cols]).astype(BF)
            for h in range(kb):
                u = t[:, _head(h)]
                if i < 2:
                    u = u.astype(F32)
                    u = (u * cos + pltpu.roll(u, HEAD // 2, 1) * sin).astype(BF)
                out[here, _head(h)] = u
                if i > 0:
                    (k_s if i == 1 else v_s)[there, _head(h)] = u

    lax.fori_loop(0, bq // rows, some, None)
    e = scale * LOG2E
    top_s[...] = jnp.full(top_s.shape, NEG, F32)
    mix_s[...] = jnp.zeros(mix_s.shape, F32)

    def block(start, size, lo, masked):
        here = pl.ds(pl.multiple_of(start, size), size)
        scores = [_dot(k_s[here, _head(i)], q_ref[lo:, _head(i)], 1, 1) for i in range(kb)]
        ok = _below(size, bq - lo) if masked else None
        ones = jnp.ones((8, size), BF)
        weights, keeps = [], []
        for i, s in enumerate(scores):
            if masked:
                s = jnp.where(ok, s, HIDDEN)
            old = top_s[i : i + 1, lo:]
            top = jnp.maximum(old, s.max(axis=0, keepdims=True))
            top_s[i : i + 1, lo:] = top
            weights.append(jnp.exp2((s - top) * e).astype(BF))
            keeps.append(jnp.exp2((old - top) * e))
        for i in range(kb):
            values = jnp.concatenate([v_s[here, _head(i)].T, ones], axis=0)
            mix_s[i, :, lo:] = mix_s[i, :, lo:] * keeps[i] + _dot(values, weights[i])

    lax.fori_loop(0, iq, lambda j, _: block(j * bq, bq, 0, False), None)
    for lo in range(0, bq, STEP):
        block(iq * bq + lo, STEP, lo, True)
    for i in range(kb):
        top, total = top_s[i : i + 1, :], mix_s[i, HEAD : HEAD + 1, :]
        o_ref[:, _head(i)] = (mix_s[i, :HEAD, :] * (1 / total)).T.astype(BF)
        lse_ref[i : i + 1, :] = top * scale + jnp.log(total)
    if joined:
        rest[7][...] = (_dot(before[...], wo_ref[:cols, :]) + _dot(o_ref[...], wo_ref[cols:, :])).astype(BF)


def heads(place, a, own, other, cos, sin, part, before=None, wo=None, bq=1024, rows=512):
    tokens, d = a.shape[0], 2 * other.shape[0]
    cols = other.shape[1] // 3
    kb = cols // HEAD
    some = lambda wide: pl.BlockSpec((bq, wide), lambda n, p: (n, 0))
    mine = pl.BlockSpec((d // 2, cols), lambda n, p: (0, 2 * p[0] + part))
    whole = lambda t: pl.BlockSpec(t.shape, lambda n, p: (0, 0))
    joined = before is not None
    q, k, v, o, lse, *product = pl.pallas_call(
        functools.partial(_heads, kb=kb, bq=bq, rows=rows, scale=HEAD**-0.5, joined=joined),
        grid_spec=pltpu.PrefetchScalarGridSpec(
            num_scalar_prefetch=1,
            grid=(tokens // bq,),
            in_specs=[some(d), *[mine] * 3, whole(other), some(HEAD), some(HEAD), *([some(cols), whole(wo)] if joined else [])],
            out_specs=[*[some(cols)] * 4, pl.BlockSpec((kb, bq), lambda n, p: (0, n)), *([some(d)] if joined else [])],
            scratch_shapes=[pltpu.VMEM((d, 3 * cols), BF), pltpu.VMEM((tokens, cols), BF), pltpu.VMEM((tokens, cols), BF), pltpu.VMEM((kb, bq), F32),
                            pltpu.VMEM((kb, HEAD + 8, bq), F32)],
        ),
        out_shape=[*[jax.ShapeDtypeStruct((tokens, cols), BF)] * 4, jax.ShapeDtypeStruct((kb, tokens), F32),
                   *([jax.ShapeDtypeStruct((tokens, d), BF)] if joined else [])],
        compiler_params=_params("arbitrary"),
        cost_estimate=pl.CostEstimate(flops=6 * tokens * d * cols + 8 * cols * tokens * tokens, transcendentals=kb * tokens * tokens,
                                      bytes_accessed=2 * (tokens * d + 3 * d * cols + 4 * tokens * cols)),
        name="heads",
    )(place, a, *own, other, cos, sin, *([before, wo] if joined else []))
    return (q, k, v), (o, lse), *product


def _attend_bwd(q_ref, k_ref, v_ref, o_ref, lse_ref, d_ref, wo_ref, cq_ref, sq_ref, cos_ref, sin_ref, dq_ref, dk_ref, dv_ref, do_ref, dq_s, dk_s, dv_s, *, kb, bq, scale):
    iq = pl.program_id(0)
    e = scale * LOG2E

    @pl.when(iq == 0)
    def _():
        dk_s[...] = jnp.zeros_like(dk_s)
        dv_s[...] = jnp.zeros_like(dv_s)

    dq_s[...] = jnp.zeros_like(dq_s)
    do_ref[...] = _dot(d_ref[...], wo_ref[...], 1, 1).astype(BF)
    lses = [lse_ref[i : i + 1, :] * LOG2E for i in range(kb)]
    deltas = [(do_ref[:, _head(i)].astype(F32) * o_ref[:, _head(i)].astype(F32)).T.sum(axis=0, keepdims=True) for i in range(kb)]

    def block(start, size, lo, masked):
        here = pl.ds(pl.multiple_of(start, size), size)
        scores = [_dot(k_ref[here, _head(i)], q_ref[lo:, _head(i)], 1, 1) for i in range(kb)]
        dps = [_dot(v_ref[here, _head(i)], do_ref[lo:, _head(i)], 1, 1) for i in range(kb)]
        ok = _below(size, bq - lo) if masked else None
        for i in range(kb):
            p = jnp.exp2(scores[i] * e - lses[i][:, lo:])
            if masked:
                p = jnp.where(ok, p, 0.0)
            ds = (p * (dps[i] - deltas[i][:, lo:])).astype(BF)
            dv_s[i, here, :] += _dot(p.astype(BF), do_ref[lo:, _head(i)])
            dk_s[i, here, :] += _dot(ds, q_ref[lo:, _head(i)])
            dq_s[i, :, lo:] += _dot(k_ref[here, _head(i)].T, ds)

    lax.fori_loop(0, iq, lambda j, _: block(j * bq, bq, 0, False), None)
    for lo in range(0, bq, STEP):
        block(iq * bq + lo, STEP, lo, True)
    for i in range(kb):
        d = (dq_s[i] * scale).T
        dq_ref[:, _head(i)] = (d * cq_ref[...] + pltpu.roll(d * sq_ref[...], HEAD // 2, 1)).astype(BF)

    @pl.when(iq == pl.num_programs(0) - 1)
    def _():
        for i in range(kb):
            def some(n, _):
                here = pl.ds(pl.multiple_of(n * bq, bq), bq)
                d = dk_s[i, here, :] * scale
                dk_ref[here, _head(i)] = (d * cos_ref[here, :] + pltpu.roll(d * sin_ref[here, :], HEAD // 2, 1)).astype(BF)
                dv_ref[here, _head(i)] = dv_s[i, here, :].astype(BF)

            lax.fori_loop(0, dk_ref.shape[0] // bq, some, None)


def attend_bwd(q, k, v, o, lse, d, wo, cos, sin, part, bq=512):
    tokens, cols = q.shape
    kb = lse.shape[0]
    width = d.shape[1]
    some = pl.BlockSpec((bq, cols), lambda n: (n, 0))
    keys = pl.BlockSpec((tokens, cols), lambda n: (0, 0))
    near = pl.BlockSpec((bq, HEAD), lambda n: (n, 0))
    whole = pl.BlockSpec((tokens, HEAD), lambda n: (0, 0))
    return pl.pallas_call(
        functools.partial(_attend_bwd, kb=kb, bq=bq, scale=HEAD**-0.5),
        grid=(tokens // bq,),
        in_specs=[some, keys, keys, some, pl.BlockSpec((kb, bq), lambda n: (0, n)), pl.BlockSpec((bq, width), lambda n: (n, 0)),
                  pl.BlockSpec((cols, width), lambda n: (part, 0)), near, near, whole, whole],
        out_specs=[some, keys, keys],
        out_shape=[jax.ShapeDtypeStruct(q.shape, BF)] * 3,
        scratch_shapes=[pltpu.VMEM((bq, cols), BF), pltpu.VMEM((kb, HEAD, bq), F32), pltpu.VMEM((kb, tokens, HEAD), F32), pltpu.VMEM((kb, tokens, HEAD), F32)],
        compiler_params=_params("arbitrary"),
        cost_estimate=pl.CostEstimate(flops=16 * cols * tokens * tokens, transcendentals=kb * tokens * tokens, bytes_accessed=16 * tokens * cols),
        name="attend_bwd",
    )(q, k, v, o, lse, d, wo, cos, sin, cos, sin)


def _mlp(place_ref, b_ref, dy_ref, go, uo, gr, ur, dn_ref, *rest, rows, given, begun):
    sums, rest = (rest[:4], rest[4:]) if given else (None, rest)
    db_in, rest = (rest[0], rest[1:]) if begun else (None, rest)
    db_ref, dg_ref, du_ref, dd_ref, dother_ref, gate_s, up_s, dg_s, du_s, dd_s, db_s = rest
    n, place = pl.program_id(0), place_ref[0]
    tokens, d = b_ref.shape
    half = d // 2
    mine, theirs = pl.ds(pl.multiple_of(place * half, half), half), pl.ds(pl.multiple_of((1 - place) * half, half), half)

    @pl.when(n == 0)
    def _():
        db_s[...] = db_in[...] if begun else jnp.zeros_like(db_s)

    dg_s[...] = jnp.zeros_like(dg_s)
    du_s[...] = jnp.zeros_like(du_s)
    dd_s[...] = sums[2][...] if given else jnp.zeros_like(dd_s)
    _whole(gate_s, go[...], gr[...], place)
    _whole(up_s, uo[...], ur[...], place)
    gate_t, up_t = gate_s[...].T, up_s[...].T

    def first(m):
        here = pl.ds(m * rows, rows)
        b, dy = b_ref[here, :], dy_ref[here, :]
        g = _dot(gate_t, b, 1, 1)
        u = _dot(up_t, b, 1, 1)
        dh = _dot(dn_ref[...], dy, 1, 1).astype(BF).astype(F32)
        s = 0.5 * jnp.tanh(0.5 * g) + 0.5
        silu = g * s
        return (silu * u).astype(BF), (dh * u * (s + silu * (1 - s))).astype(BF), (dh * silu).astype(BF)

    def second(m, hidden, dg, du):
        here = pl.ds(m * rows, rows)
        b, dy = b_ref[here, :], dy_ref[here, :]
        dd_s[...] += _dot(hidden, dy)
        dg_s[...] += _dot(dg, b)
        du_s[...] += _dot(du, b)
        db_s[:, here] += _dot(gate_s[...], dg) + _dot(up_s[...], du)

    now = first(0)
    for m in range(tokens // rows):
        then = first(m + 1) if m + 1 < tokens // rows else None
        second(m, *now)
        now = then

    for i, (s, out) in enumerate(((dg_s, dg_ref), (du_s, du_ref))):
        t = s[...].T
        s_own = jnp.where(place == 0, t[:half], t[half:])
        s_other = jnp.where(place == 0, t[half:], t[:half])
        out[...] = ((s_own + sums[i][...]) if given else s_own).astype(out.dtype)
        dother_ref[i] = ((s_other + sums[3][i]) if given else s_other).astype(dother_ref.dtype)
    dd_ref[...] = dd_s[...].astype(dd_ref.dtype)

    @pl.when(n == pl.num_programs(0) - 1)
    def _():
        db_ref[...] = db_s[...].T.astype(BF) if begun else db_s[...]


def mlp(place, b, dy, at, gate, up, other, down, part, sums=None, db=None, results=None, units=512, rows=512):
    tokens, d = b.shape
    hidden = down.shape[0] // 2
    steps = hidden // units
    final = sums is not None
    kind = BF if final else F32
    given = [*(sums or []), *([db] if db is not None else [])]
    kept = list(results) if results is not None else []
    whole = pl.BlockSpec((tokens, d), lambda n, p: (0, 0))
    whole_t = pl.BlockSpec((d, tokens), lambda n, p: (0, 0))
    own = pl.BlockSpec((d // 2, units), lambda n, p: (0, (2 * p[0] + part) * steps + n))
    got = [pl.BlockSpec((d // 2, units), functools.partial(lambda i, n, p: (0, i * steps + n), i)) for i in range(2)]
    w = pl.BlockSpec((d // 2, units), lambda n, p: (0, n))
    w2 = pl.BlockSpec((2, d // 2, units), lambda n, p: (0, 0, n))
    wd = pl.BlockSpec((units, d), lambda n, p: (n, 0))
    wd_in = pl.BlockSpec((units, d), lambda n, p: (part * steps + n, 0))
    shape = jax.ShapeDtypeStruct
    full = gate.shape if final else (d // 2, hidden)
    first = 8 + len(given)

    def kernel(*refs):
        _mlp(*refs[:first], *refs[first + len(kept) :], rows=rows, given=final, begun=db is not None)

    out, *dw = pl.pallas_call(
        kernel,
        grid_spec=pltpu.PrefetchScalarGridSpec(
            num_scalar_prefetch=1,
            grid=(steps,),
            in_specs=[whole, pl.BlockSpec((tokens, d), lambda n, p: (0, at)), own, own, *got, wd_in, *([w, w, wd, w2] if final else []), *([whole_t] if db is not None else []),
                      *[pl.BlockSpec(memory_space=pl.ANY)] * len(kept)],
            out_specs=[whole if db is not None else whole_t, *([own, own, wd_in] if final else [w, w, wd]), w2],
            scratch_shapes=[pltpu.VMEM((d, units), BF)] * 2 + [pltpu.VMEM((units, d), F32)] * 3 + [pltpu.VMEM((d, tokens), F32)],
        ),
        out_shape=[shape((tokens, d), BF) if db is not None else shape((d, tokens), F32), shape(full, kind), shape(full, kind),
                   shape((2 * hidden if final else hidden, d), kind), shape((2, d // 2, hidden), kind)],
        input_output_aliases={first + i: 1 + i for i in range(len(kept))},
        compiler_params=_params("arbitrary"),
        cost_estimate=pl.CostEstimate(flops=16 * tokens * d * hidden, transcendentals=tokens * hidden, bytes_accessed=30 * d * hidden),
        name="mlp",
    )(place, b, dy, gate, up, other, other, down, *given, *kept)
    return out, dw


def _states_bwd(place_ref, *refs, begun, last):
    halves = (len(refs) - 5 - begun) // 4
    ds, (qo, ko, vo), others = refs[: 3 * halves], refs[3 * halves : 3 * halves + 3], refs[3 * halves + 3 : 4 * halves + 3]
    da_ref, w_s = refs[-2:]
    cols = ds[0].shape[1]

    @pl.when(pl.program_id(0) == 0)
    def _():
        for h in range(halves):
            for i, own in enumerate((qo, ko, vo)):
                part = slice((3 * h + i) * cols, (3 * h + i + 1) * cols)
                _whole(w_s.at[:, part], own[:, h * cols : (h + 1) * cols], others[h][:, i * cols : (i + 1) * cols], place_ref[0])

    da = sum(_dot(t[...], w_s[:, n * cols : (n + 1) * cols], 1, 1) for n, t in enumerate(ds))
    if begun:
        da += refs[-3][...]
    da_ref[...] = da.astype(BF) if last else da


def states_bwd(place, ds, own, others, parts=(0, 1), da=None, rows=512):
    tokens, cols = ds[0].shape
    d = 2 * own[0].shape[0]
    last = len(parts) == 2 or da is not None
    some = lambda wide: pl.BlockSpec((rows, wide), lambda n, p: (n, 0))
    mine = pl.BlockSpec((d // 2, len(parts) * cols), (lambda n, p: (0, p[0])) if len(parts) == 2 else (lambda n, p: (0, 2 * p[0] + parts[0])))
    whole = pl.BlockSpec(others[0].shape, lambda n, p: (0, 0))
    given = [] if da is None else [da]
    return pl.pallas_call(
        functools.partial(_states_bwd, begun=len(given), last=last),
        grid_spec=pltpu.PrefetchScalarGridSpec(
            num_scalar_prefetch=1,
            grid=(tokens // rows,),
            in_specs=[*[some(cols)] * len(ds), *[mine] * 3, *[whole] * len(parts), *[some(d)] * len(given)],
            out_specs=some(d),
            scratch_shapes=[pltpu.VMEM((d, 3 * len(parts) * cols), BF)],
        ),
        out_shape=jax.ShapeDtypeStruct((tokens, d), BF if last else F32),
        compiler_params=_params("arbitrary"),
        cost_estimate=pl.CostEstimate(flops=6 * len(parts) * tokens * d * cols, transcendentals=0, bytes_accessed=2 * (tokens * d + 3 * len(parts) * (d + tokens) * cols)),
        name="states_bwd",
    )(place, *ds, *own, *others, *given)


def _weights_bwd(place_ref, a_ref, dq_ref, dk_ref, dv_ref, *rest, given):
    sums, rest = (rest[:4], rest[4:]) if given else (None, rest)
    outs, dother_ref, accs = rest[:3], rest[3], rest[4:]
    n, place = pl.program_id(0), place_ref[0]
    half, cols = a_ref.shape[1] // 2, dq_ref.shape[1]
    mine, theirs = pl.ds(pl.multiple_of(place * half, half), half), pl.ds(pl.multiple_of((1 - place) * half, half), half)
    part = [slice(i * cols, (i + 1) * cols) for i in range(3)]

    @pl.when(n == 0)
    def _():
        for i, s in enumerate(accs):
            if given:
                s[mine, :] = sums[i][...]
                s[theirs, :] = sums[3][:, part[i]]
            else:
                s[...] = jnp.zeros_like(s)

    a_t = a_ref[...].T
    for s, t in zip(accs, (dq_ref, dk_ref, dv_ref)):
        s[...] += _dot(a_t, t[...])

    @pl.when(n == pl.num_programs(0) - 1)
    def _():
        for i, s in enumerate(accs):
            outs[i][...] = s[mine, :].astype(outs[i].dtype)
            dother_ref[:, part[i]] = s[theirs, :].astype(dother_ref.dtype)


def weights_bwd(place, a, ds, d, part, sums=None, results=None, rows=1024):
    tokens, cols = ds[0].shape
    final = sums is not None
    kind = BF if final else F32
    given = list(sums) if final else []
    kept = list(results) if results is not None else []
    some = lambda wide: pl.BlockSpec((rows, wide), lambda n, p: (n, 0))
    mine = pl.BlockSpec((d // 2, cols), lambda n, p: (0, 2 * p[0] + part))
    w = pl.BlockSpec((d // 2, cols), lambda n, p: (0, 0))
    w3 = pl.BlockSpec((d // 2, 3 * cols), lambda n, p: (0, 0))
    shape = jax.ShapeDtypeStruct
    full = (d // 2, 4 * cols) if final else (d // 2, cols)
    first = 5 + len(given)

    def kernel(*refs):
        _weights_bwd(*refs[:first], *refs[first + len(kept) :], given=final)

    return pl.pallas_call(
        kernel,
        grid_spec=pltpu.PrefetchScalarGridSpec(
            num_scalar_prefetch=1,
            grid=(tokens // rows,),
            in_specs=[some(d), *[some(cols)] * 3, *([w, w, w, w3] if final else []), *[pl.BlockSpec(memory_space=pl.ANY)] * len(kept)],
            out_specs=[*[mine if final else w] * 3, w3],
            scratch_shapes=[pltpu.VMEM((d, cols), F32)] * 3,
        ),
        out_shape=[*[shape(full, kind)] * 3, shape((d // 2, 3 * cols), kind)],
        input_output_aliases={first + i: i for i in range(len(kept))},
        compiler_params=_params("arbitrary"),
        cost_estimate=pl.CostEstimate(flops=6 * tokens * d * cols, transcendentals=0, bytes_accessed=2 * (tokens * d + 6 * d * cols + 3 * tokens * cols)),
        name="weights_bwd",
    )(place, a, *ds, *given, *kept)


def normed(h):
    wide = h.astype(F32)
    scale = lax.rsqrt(jnp.mean(wide**2, -1, keepdims=True) + 1e-6)
    return (wide * scale).astype(BF)


def tables(tokens):
    half = HEAD // 2
    angle = jnp.arange(tokens, dtype=F32)[:, None] * THETA ** (-jnp.arange(half, dtype=F32) / half)
    cos, sin = jnp.cos(angle), jnp.sin(angle)
    return jnp.concatenate([cos, cos], 1), jnp.concatenate([-sin, sin], 1)


def after(t, *those):
    return lax.optimization_barrier((t, *those))[0]


def solution(mesh):
    swap = [(0, 1), (1, 0)]
    everyone = ("tp", "dp")

    def step(x, dy, wq, wk, wv, wo, wg, wu, wd):
        p = lax.axis_index("dp")
        place = p.astype(jnp.int32)[None]
        x, dy = x[0], dy[0]
        tokens = x.shape[0] * mesh.shape["tp"]

        def halves(t, axis, n):
            size = t.shape[axis] // 2
            return lax.dynamic_slice_in_dim(t, n * size, size, axis)

        def by_place(mine, theirs):
            return jnp.where(p == 0, mine, theirs), jnp.where(p == 0, theirs, mine)

        def gather(t):
            return lax.all_gather(t, everyone, axis=0, tiled=True)

        def collect(part):
            return lax.psum_scatter(part, everyone, scatter_dimension=0, tiled=True)

        def plus(t, more):
            return (t.astype(F32) + more.astype(F32)).astype(BF)

        def to_send(ws, part):
            size = ws[0].shape[1] // 4
            return jnp.concatenate([lax.dynamic_slice_in_dim(w, (2 * (1 - p) + part) * size, size, 1) for w in ws], 1)

        own, own2 = (wq, wk, wv), (wg, wu)
        send = [to_send(own, n) for n in (0, 1)]
        send2 = [to_send(own2, n) for n in (0, 1)]
        got = lax.ppermute(jnp.concatenate([halves(t, 0, 1 - p) for t in (x, dy)], 1), "dp", swap)
        got = jnp.split(after(got, *send), 2, 1)
        xs, dys = (by_place(halves(t, 0, p), more) for t, more in zip((x, dy), got))
        norms, backs = zip(*(jax.vjp(normed, t) for t in xs))
        a = [gather(norms[0]), gather(jnp.concatenate([norms[1], dys[0]], 1))]
        other = [lax.ppermute(send[0], "dp", swap)]
        other.append(lax.ppermute(after(send[1], a[0]), "dp", swap))
        cos, sin = tables(tokens)

        def half_heads(a, n, *more):
            return heads(place, a, own, other[n], cos, sin, n, *more)

        t00, o00 = half_heads(after(a[0], norms[1], dys[0], send2[0]), 0)
        other2 = []
        for n in (0, 1):
            other2.append(lax.ppermute(after(send2[n], o00[0]), "dp", swap))
        t01, o01, h0 = half_heads(a[0], 1, o00[0], wo)
        h0 = collect(after(h0, a[1]))
        dy1 = gather(after(dys[1], h0))
        t10, o10 = half_heads(after(a[1], o01[0]), 0)
        h0 = plus(xs[0], after(h0, o10[0]))
        b0, back0 = jax.vjp(normed, h0)
        t11, o11, h1 = half_heads(after(a[1], b0), 1, o10[0], wo)
        b0 = gather(b0)
        h1 = collect(h1)
        db0, w0a = mlp(place, b0, a[1], 1, wg, wu, other2[0], wd, 0)
        h1 = plus(xs[1], after(h1, db0))
        b1, back1 = jax.vjp(normed, h1)
        db0, w0b = mlp(place, after(b0, b1), a[1], 1, wg, wu, other2[1], wd, 1, None, db0)
        b1 = gather(b1)
        db0 = collect(db0)
        db1, w1a = mlp(place, b1, dy1, 0, wg, wu, other2[0], wd, 0, w0a)
        ga = lax.ppermute(w1a[3], "dp", swap)
        dh0 = plus(dys[0], back0(after(db0, db1))[0])
        db1, w1b = mlp(place, after(b1, dh0), dy1, 0, wg, wu, other2[1], wd, 1, w0b, db1, w1a[:3])
        d0 = gather(dh0)
        gb = lax.ppermute(w1b[3], "dp", swap)
        db1 = collect(db1)

        def heads_back(t, o, d, n):
            return attend_bwd(*t, *o, d, wo, cos, sin, n)

        ds0 = heads_back(t00, o00, d0, 0)
        dh1 = plus(dys[1], back1(after(db1, ds0[0]))[0])
        ds1 = heads_back((after(t01[0], dh1), *t01[1:]), o01, d0, 1)
        d1 = gather(dh1)
        da0 = collect(after(states_bwd(place, [*ds0, *ds1], own, other), d1))
        s0, s1 = (weights_bwd(place, a[0], t, x.shape[1], n) for n, t in enumerate((ds0, ds1)))
        ds0 = heads_back(t10, o10, after(d1, s0[3], s1[3]), 0)
        da1 = states_bwd(place, ds0, own, other[:1], (0,))
        s0 = weights_bwd(place, a[1], ds0, x.shape[1], 0, s0)
        g0 = lax.ppermute(s0[3], "dp", swap)
        ds1 = heads_back((after(t11[0], s0[3], da1), *t11[1:]), o11, d1, 1)
        da1 = states_bwd(place, ds1, own, other[1:], (1,), da1)
        s1 = weights_bwd(place, after(a[1], da1), ds1, x.shape[1], 1, s1, s0[:3])
        da1 = collect(da1)
        g1 = lax.ppermute(s1[3], "dp", swap)
        dx0 = plus(dh0, backs[0](da0)[0])
        dx1 = plus(dh1, backs[1](da1)[0])
        mine, theirs = by_place(dx0, dx1)
        theirs = lax.ppermute(theirs, "dp", swap)
        dx = jnp.concatenate(by_place(mine, theirs), 0)
        dwo = jnp.concatenate([(_dot(m[0], d0, 0, 0) + _dot(n[0], d1, 0, 0)).astype(BF) for m, n in ((o00, o10), (o01, o11))], 0)

        def with_other(full, *got):
            size = got[0].shape[1]
            for n, t in enumerate(got):
                full = lax.dynamic_update_slice(full, t, (0, (2 * (1 - p) + n) * size))
            return full

        cols = g0.shape[1] // 3
        dw = [with_other(s1[i], *(g[:, i * cols : (i + 1) * cols] for g in (g0, g1))) for i in range(3)]
        ga, gb = after(ga, s1[3]), after(gb, s1[3])
        dwg, dwu = (with_other(w1b[i], ga[i], gb[i]) for i in range(2))
        return (dx[None], *dw, dwo, dwg, dwu, w1b[2])

    states, by_columns, by_rows = P("dp", "tp", None), P("dp", "tp"), P(("tp", "dp"), None)
    weights = (by_columns, by_columns, by_columns, by_rows, by_columns, by_columns, by_rows)
    return jax.shard_map(step, mesh=mesh, in_specs=(states, states, *weights), out_specs=(states, *weights), check_vma=False)
```
